32 devices in a mesh: sim: 2 (over y), band: 4 (over z), ord: 4 (over x, core).
Axes of the slice: x: 2, y: 2, z: 4, core: 2. Of those that a mesh axis runs over, the one named last changes fastest.
Arguments:
- alm: bfloat16 [12, 256, 8192], P('sim', 'ord', 'band'), parts along dimension 0, may hold values from -6 to 6
- legendre: bfloat16 [16, 256, 8192], P(None, 'ord', 'band'), may hold values from -0.005859375 to 0.005859375
- order_ids: int32 [256], P('ord'), may hold values from 0 to 8191, as said below
- cycle_number: int32 [16], P('band'), may hold values from 1 to 32767
- src_band: int32 [4096, 1], P(('sim', 'band', 'ord')), parts along dimension 0, may hold values from 0 to 3; in each aligned block of 128 rows (0 to 127, 128 to 255, ...) at most 64 rows name the same one
- src_block: int32 [4096], P(('sim', 'band', 'ord')), parts along dimension 0, may hold values from 0 to 127
- weights: bfloat16 [4096, 128, 128], P(('sim', 'band', 'ord')), parts along dimension 0, may hold values from -0.5 to 0.5
Outputs:
- sky_map: bfloat16 [6, 16, 16384], P('sim', 'band', 'ord'), parts along dimension 0
- lensed: float32 [6, 16, 16384], P('sim', 'band', 'ord'), parts along dimension 0
The draws below stay inside these ranges and needn't reach their ends.
There are 2 independent parts, one for each index of `sim`. The reference program is written for one: setup_inputs(seed, part) draws one part's arguments, and reference() takes and returns one part's arrays. A program takes and returns all parts, laid end to end along the dimension named above; an argument that names none is the same for every part. Nothing has to cross between parts.
Inputs may be any that keep to these rules, and one draw needn't show every extreme that they name: `src_band`: among the blocks of one device at most 64 name the same band, a bound that some block reaches. `order_ids`: distinct values; one of them is 0.
All inputs are finite; a program needn't handle non-finite values.
Results may differ from the reference program's by a relative error of at most 0.0029.
Values may be sent and summed in bfloat16 or wider, within the bound.
No kernel may reach another device: no remote copies, remote signals or barrier semaphores. Data moves between devices by JAX's collectives and lax.ppermute only.
A program may use at most 128 MiB of HBM per device.

```python
import math
import jax
import jax.numpy as jnp
import numpy as np
from jax import lax

L = 8192
NPIX = 16384
BLK = 128
CYCLE_DEV = 4
CYCLES = 16
MO = 256
NB_DEV = 128
CAP = 64
N_BAND = 4
N_ORD = 4


def draw_order_ids(key, part):
    others = jax.random.permutation(jax.random.fold_in(key, 11), NPIX // 2 - 1)[:MO].astype(jnp.int32) + 1
    zero_slot = jax.random.randint(jax.random.fold_in(key, 23), (), 0, MO).astype(jnp.int32)
    return others.at[zero_slot].set(0).astype(jnp.int32)


def with_ends(array, own_key, smallest, top_value):
    longest = array.shape.index(max(array.shape))
    spots = []
    for shift in (0, 1):
        where = [jax.random.randint(jax.random.fold_in(own_key, axis), (), 0, length) for axis, length in enumerate(array.shape)]
        where[longest] = (where[longest] + shift) % array.shape[longest]
        spots.append(tuple(where))
    return array.at[spots[0]].set(smallest).at[spots[1]].set(top_value)


def strengthened(array, key, source, target, blocks, factor):
    def block_of(dim):
        return (jnp.arange(array.shape[dim]) // (array.shape[dim] // blocks)).reshape((-1,) + (1,) * (array.ndim - 1 - dim))

    first = jax.random.permutation(key, blocks)[block_of(target)]
    other_side = (block_of(target) + blocks // 2) % blocks
    return jnp.where((block_of(source) == first) | (block_of(source) == other_side), factor * array, array)


def levels(key, extent, pieces, low, top_value):
    gain, own = 1.0, jax.random.fold_in(key, 6)
    for position, blocks in pieces:
        heights = jnp.exp(jax.random.uniform(jax.random.fold_in(own, position), (blocks,), jnp.float32, low / len(pieces), top_value / len(pieces)))
        gain = gain * jnp.repeat(heights, extent[position] // blocks).reshape([-1 if axis == position else 1 for axis in range(len(extent))])
    return gain


def assign_block(stream_key, own, number, rows, number_of, top, bound, slope):
    order = jax.random.permutation(stream_key, number_of)
    heavy_load, usual = portions_of(number_of, rows * top, bound, slope, True), portions_of(number_of, rows * top, bound, slope, False)
    places = jnp.arange(number_of)

    def named(lengths, offset_by):
        used = int((lengths > 0).sum())
        fixed = max(1, used // 4)
        passed = fixed + (places - fixed + offset_by * (used - fixed)) % max(1, number_of - fixed)
        return jnp.zeros((number_of,), jnp.int32).at[order[jnp.where(places < fixed, places, passed)]].set(jnp.asarray(lengths, jnp.int32))

    lengths = jnp.where(number % 4 == 0, named(heavy_load, number // 4), named(usual, number - number // 4 - 1))
    mixed = jax.random.permutation(jax.random.fold_in(own, 3), number_of)
    giver, receiver = mixed[0:number_of // 2 * 2:2], mixed[1:number_of // 2 * 2:2]
    slack = jnp.minimum(lengths[giver] - 1, bound - lengths[receiver]) // 2
    slack = jnp.where((giver == order[0]) | (receiver == order[0]) | (lengths[receiver] == 0), 0, jnp.maximum(slack, 0))
    passed = jax.random.randint(jax.random.fold_in(own, 4), (number_of // 2,), 0, 1 << 20) % (slack + 1)
    lengths = lengths.at[giver].add(-passed).at[receiver].add(passed)
    labels = jnp.searchsorted(jnp.cumsum(lengths), jnp.arange(rows * top), side="right").astype(jnp.int32)
    listing = labels.reshape(top, rows).T
    listing = listing[jax.random.permutation(jax.random.fold_in(own, 1), rows)]
    offset_by = jax.random.randint(jax.random.fold_in(own, 2), (rows, 1), 0, top)
    return jnp.take_along_axis(listing, (jnp.arange(top)[None, :] + offset_by) % top, axis=1)


def portions_of(number_of, total, limit, slope, full):
    loads = [(1 << 20) // math.isqrt(standing ** slope) + 1 for standing in range(1, number_of + 1)]
    largest = limit if full else min(limit, max(-(-total // number_of), total * loads[0] // sum(loads)))
    least = 1 if total - largest >= number_of - 1 else 0
    holding, rest = [largest] + [least] * (number_of - 1), total - largest - least * (number_of - 1)
    while rest > 0:
        candidates = [i for i in range(1, number_of) if holding[i] < largest] or [i for i in range(1, number_of) if holding[i] < limit]
        pool, remaining = sum([loads[i] for i in candidates]), rest
        for i in candidates:
            extra = min(limit - holding[i], max(1, remaining * loads[i] // pool), rest)
            holding[i] = holding[i] + extra
            rest = rest - extra
    return np.array(holding)


def centred(key, shape, deviation, most, shards=(), kind=jnp.bfloat16):
    values = deviation * jax.random.normal(key, shape, jnp.float32)
    if shards:
        values = values * levels(key, shape, shards, -0.22, 0.18)
    return jnp.clip(values, -most, most).astype(kind)


def heavy_noise(rng, shape, spread, bound, split, heavy, held_as=jnp.bfloat16):
    values = spread * jax.random.normal(rng, shape, jnp.float32)
    if split:
        values = values * levels(rng, shape, split, -0.22, 0.18)
    return jnp.clip(strengthened(values, jax.random.fold_in(rng, 3), *heavy), -bound, bound).astype(held_as)


def setup_inputs(seed: int = 0, part: int = 0) -> dict:
    key_of = jax.random.split(jax.random.key(seed), 8)
    part_splits = jax.random.split(jax.random.fold_in(key_of[7], part), 8)
    alm = centred(part_splits[0], (6, MO, L), 1.0, 6.0, ((1, 4), (2, 4)))
    legendre = heavy_noise(key_of[1], (CYCLES, MO, L), (L * MO) ** -0.5, 0.005859375, ((1, 4), (2, 4)), (2, 0, 4, 2.0))
    order_ids = draw_order_ids(jax.random.fold_in(key_of[7], 71), part)
    cycle_number = with_ends(jax.random.randint(key_of[3], (CYCLES,), 1, 2 * NPIX), jax.random.fold_in(key_of[3], 1), 1, (2 * NPIX) - 1).astype(jnp.int32)
    src_band_keys = jax.random.split(jax.random.fold_in(part_splits[4], 1), (NB_DEV * N_BAND * N_ORD) // NB_DEV)
    src_band_turns = jax.random.permutation(jax.random.fold_in(part_splits[4], 3), (NB_DEV * N_BAND * N_ORD) // NB_DEV)
    src_band = jax.vmap(lambda own, number: assign_block(jax.random.fold_in(part_splits[4], 2), own, number, NB_DEV, N_BAND, 1, CAP, 2))(src_band_keys, src_band_turns).reshape((NB_DEV * N_BAND * N_ORD, 1))
    src_block = with_ends(jax.random.randint(part_splits[5], (NB_DEV * N_BAND * N_ORD,), 0, NB_DEV), jax.random.fold_in(part_splits[5], 1), 0, NB_DEV - 1).astype(jnp.int32)
    weights = centred(part_splits[6], (NB_DEV * N_BAND * N_ORD, BLK, BLK), BLK ** -0.5, 0.5, ((0, 16),))
    return dict(alm=alm, legendre=legendre, order_ids=order_ids, cycle_number=cycle_number, src_band=src_band, src_block=src_block, weights=weights)


def rotate(coeffs, order_ids, cycle_number):
    parity = (cycle_number % 2).astype(jnp.float32)
    orders = order_ids.astype(jnp.float32)
    angle = (math.pi / NPIX) * orders[None, :] * parity[:, None]
    cosine = jnp.cos(angle)[:, None, :]
    sine = jnp.sin(angle)[:, None, :]
    factor = jnp.where(order_ids == 0, 1.0, 2.0).astype(jnp.float32)[None, None, :]
    real_part = coeffs[:, 0:3, :]
    imag_part = coeffs[:, 3:6, :]
    rot_re = factor * (real_part * cosine - imag_part * sine)
    rot_im = factor * (real_part * sine + imag_part * cosine)
    return rot_re, rot_im


def synthesize(rot_re, rot_im, order_ids, columns):
    phase = (order_ids[:, None] * columns[None, :]) % NPIX
    angle = phase.astype(jnp.float32) * (2.0 * math.pi / NPIX)
    right = jnp.concatenate([jnp.cos(angle), jnp.sin(angle)], axis=0)
    cycles = rot_re.shape[0]
    left = jnp.concatenate([rot_re, -rot_im], axis=2).reshape(cycles * 3, -1)
    pixels = jnp.dot(left, right, precision=lax.Precision.HIGHEST, preferred_element_type=jnp.float32)
    return jnp.transpose(pixels.reshape(cycles, 3, -1), (1, 0, 2))


def reference(alm, legendre, order_ids, cycle_number, src_band, src_block, weights):
    def one_order(index):
        rows = lax.dynamic_index_in_dim(legendre, index, 1, keepdims=False)
        terms = lax.dynamic_index_in_dim(alm, index, 1, keepdims=False)
        return jnp.dot(rows, terms.T, preferred_element_type=jnp.float32)

    per_order = lax.map(one_order, jnp.arange(MO, dtype=jnp.int32))
    coeffs = jnp.transpose(per_order, (1, 2, 0))
    rot_re, rot_im = rotate(coeffs, order_ids, cycle_number)
    columns = jnp.arange(NPIX, dtype=jnp.int32)
    sky_map = synthesize(rot_re, rot_im, order_ids, columns).astype(jnp.bfloat16)
    npix_here = NPIX // N_ORD
    blocks = sky_map.reshape(3, N_BAND, CYCLE_DEV, N_ORD, npix_here)
    blocks = jnp.transpose(blocks, (0, 1, 3, 2, 4)).reshape(3, N_BAND, N_ORD, NB_DEV, BLK)
    source_band = src_band[:, 0].reshape(N_BAND, N_ORD, NB_DEV)
    source_index = src_block.reshape(N_BAND, N_ORD, NB_DEV)
    ord_index = jnp.arange(N_ORD, dtype=jnp.int32)[None, :, None]
    source = blocks[:, source_band, ord_index, source_index, :]
    source = jnp.transpose(source, (1, 2, 0, 3, 4)).reshape(N_BAND * N_ORD, 3, NB_DEV, BLK)
    matrices = weights.reshape(N_BAND * N_ORD, NB_DEV, BLK, BLK)

    def one_device(pair):
        mats, values = pair
        return jnp.einsum("kij,ckj->cki", mats.astype(jnp.float32), values.astype(jnp.float32))

    lensed = lax.map(one_device, (matrices, source))
    lensed = lensed.reshape(N_BAND, N_ORD, 3, CYCLE_DEV, npix_here)
    lensed = jnp.transpose(lensed, (2, 0, 3, 1, 4)).reshape(3, N_BAND * CYCLE_DEV, NPIX)
    return sky_map, lensed
```

```python
import functools
import math

import jax
import jax.numpy as jnp
from jax import lax
from jax.experimental import pallas as pl
from jax.experimental.pallas import tpu as pltpu
from jax.sharding import PartitionSpec as P

LANES = 128
GROUP = 16
NT = (((1,), (1,)), ((), ()))
SINE = (6.2831851600887045, -41.34165503125142, 81.60100406374923, -76.54978209038376, 39.53670461908883)


def sin_turns(v):
    z = v * v
    total = SINE[-1]
    for term in SINE[-2::-1]:
        total = total * z + term
    return total * v


def wrap(u):
    return u - jnp.round(u)


def cos_turns(u):
    return sin_turns(0.25 - jnp.abs(u))


def split(x):
    high = x.astype(jnp.bfloat16)
    return high, (x - high.astype(jnp.float32)).astype(jnp.bfloat16)


def analysis(band_ref, cycle_ref, orders_ref, legendre_hbm, alm_hbm, out_ref, legendre, alm, sems):
    cycles, orders, _ = legendre.shape
    parts = alm.shape[0]
    half = parts // 2
    groups = orders // GROUP
    copies = []
    for g in range(groups):
        rows = pl.ds(g * GROUP, GROUP)
        pair = (
            pltpu.make_async_copy(alm_hbm.at[:, rows], alm.at[:, rows], sems.at[0, g]),
            pltpu.make_async_copy(legendre_hbm.at[:, rows], legendre.at[:, rows], sems.at[1, g]),
        )
        for copy in pair:
            copy.start()
        copies.append(pair)

    band = band_ref[0]
    cycles_here = cycle_ref.shape[0]
    row = lax.broadcasted_iota(jnp.int32, (cycles, LANES // 2), 0)
    parity = jnp.zeros((cycles, LANES // 2), jnp.float32)
    for i in range(cycles_here):
        odd = (cycle_ref[i] % 2).astype(jnp.float32)
        parity = jnp.where(row == band * cycles_here + i, odd, parity)
    ids = orders_ref[...].astype(jnp.float32) * jnp.where(band == 0, 1.0, 0.0)
    base = half * 2 * orders
    out_ref[:, base : base + orders] = jnp.broadcast_to(ids, (cycles, orders))
    out_ref[:, base + orders : base + 2 * orders] = parity

    width = parts * GROUP
    rows_of = lax.broadcasted_iota(jnp.int32, (cycles * GROUP, width), 0) % GROUP
    lane_of = lax.broadcasted_iota(jnp.int32, (cycles * GROUP, width), 1) % GROUP
    same = rows_of == lane_of
    sums = []
    for g in range(groups):
        for copy in copies[g]:
            copy.wait()
        rows = slice(g * GROUP, (g + 1) * GROUP)
        left = legendre[:, rows, :].reshape(cycles * GROUP, -1)
        right = alm[:, rows, :].reshape(width, -1)
        full = lax.dot_general(left, right, NT, preferred_element_type=jnp.float32)
        full = jnp.where(same, full, 0.0)
        sums.append(jnp.sum(full.reshape(cycles, GROUP, width), axis=1))
    for f in range(half):
        pieces = [sums[g][:, c * GROUP : (c + 1) * GROUP] for c in (f, f + half) for g in range(groups)]
        out_ref[:, 2 * f * orders : 2 * (f + 1) * orders] = jnp.concatenate(pieces, axis=1)


def lens(n_ord, cycles_here, fields, place_ref, src_band_ref, src_block_ref, *refs):
    arrays = refs[:n_ord]
    weights_hbm, sky_out, lensed_out, sky, stage, weights, sem = refs[n_ord:]
    load = pltpu.make_async_copy(weights_hbm, weights, sem)
    load.start()

    band, slot = place_ref[0], place_ref[1].astype(jnp.float32)
    cycles = arrays[0].shape[0]
    half = LANES // 2
    npix_here = sky_out.shape[2]
    npix = npix_here * n_ord
    cols = npix_here // LANES
    q_len = min(512, npix_here)
    p_len = npix_here // q_len
    rows_col = fields * cycles

    lane = lax.broadcasted_iota(jnp.int32, (cycles, LANES), 1)
    low = lane < half
    low_row = low[0:1]
    meta = [a[:, fields * LANES :] for a in arrays]
    ids = [jnp.where(low_row, m[0:1], pltpu.roll(m, half, 1)[0:1]) for m in meta]
    odd = jnp.where(low, pltpu.roll(meta[0], half, 1), meta[0]) > 0.5

    q_iota = lax.broadcasted_iota(jnp.int32, (LANES, q_len), 1).astype(jnp.float32) * (1.0 / npix)
    shift = jnp.where(lax.broadcasted_iota(jnp.int32, (LANES, q_len), 0) < half, 0.0, 0.25)
    table_high, table_low = [], []
    for a in range(n_ord):
        column = jnp.broadcast_to(ids[a], (LANES, LANES)).T
        column = jnp.concatenate([column] * (q_len // LANES), axis=1)
        high, low_part = split(cos_turns(wrap(column * q_iota - shift)))
        table_high.append(high)
        table_low.append(low_part)
    table_high = jnp.concatenate(table_high, axis=0)
    table_low = jnp.concatenate(table_low, axis=0)

    p_iota = lax.broadcasted_iota(jnp.int32, (p_len, LANES), 0).astype(jnp.float32) * (q_len / npix)
    low_p = lax.broadcasted_iota(jnp.int32, (p_len, LANES), 1) < half
    left_rows = [[None] * n_ord for _ in range(p_len)]
    for a in range(n_ord):
        m = ids[a]
        factor = jnp.where(m == 0.0, 1.0, 2.0)
        start = wrap(m * (slot * (1.0 / n_ord)))
        even_turn = wrap(wrap(m * p_iota) + start)
        odd_turn = wrap(even_turn + wrap(m * (0.5 / npix)))
        terms = []
        for turn in (even_turn, odd_turn):
            cosine = cos_turns(turn) * factor
            sine = cos_turns(wrap(turn - 0.25)) * factor
            terms.append((jnp.where(low_p, cosine, -cosine), -sine))
        x = [arrays[a][:, f * LANES : (f + 1) * LANES] for f in range(fields)]
        turned = [pltpu.roll(v, half, 1) for v in x]
        for p in range(p_len):
            straight = jnp.where(odd, terms[1][0][p : p + 1], terms[0][0][p : p + 1])
            crossed = jnp.where(odd, terms[1][1][p : p + 1], terms[0][1][p : p + 1])
            left_rows[p][a] = jnp.concatenate(
                [x[f] * straight + turned[f] * crossed for f in range(fields)], axis=0
            )
    for p in range(p_len):
        high, low_part = split(jnp.concatenate(left_rows[p], axis=1))
        dot = functools.partial(jnp.dot, preferred_element_type=jnp.float32)
        pixels = dot(high, table_high) + (dot(low_part, table_high) + dot(high, table_low))
        pixels = pixels.astype(jnp.bfloat16).astype(jnp.float32)
        for j in range(q_len // LANES):
            col = p * (q_len // LANES) + j
            sky[col * rows_col : (col + 1) * rows_col, :] = pixels[:, j * LANES : (j + 1) * LANES]

    first = pl.multiple_of(band * cycles_here, cycles_here)
    for col in range(cols):
        for f in range(fields):
            own = sky[pl.ds(col * rows_col + f * cycles + first, cycles_here), :]
            sky_out[f, :, col * LANES : (col + 1) * LANES] = own.astype(jnp.bfloat16)

    stage[...] = jnp.zeros_like(stage)
    for col in range(cols):
        for c in range(cycles_here):
            k = c * cols + col
            block = src_block_ref[k]
            cycle = src_band_ref[k] * cycles_here + block // cols
            begin = (block % cols) * rows_col + cycle
            source = sky[pl.ds(begin, fields, stride=cycles), :]
            stage[2 * col + c % 2, pl.ds(c, fields, stride=cycles_here), :] = source

    load.wait()
    rows = stage.shape[1]
    cycle_of = lax.broadcasted_iota(jnp.int32, (rows, LANES), 0) % cycles_here
    for col in range(cols):
        left = jnp.concatenate([stage[2 * col], stage[2 * col + 1]], axis=1).astype(jnp.bfloat16)
        right = jnp.concatenate(
            [
                jnp.concatenate([weights[c * cols + col], weights[(c + 1) * cols + col]], axis=1)
                for c in range(0, cycles_here, 2)
            ],
            axis=0,
        )
        full = lax.dot_general(left, right, NT, preferred_element_type=jnp.float32)
        out = full[:, 0:LANES]
        for n in range(1, cycles_here // 2):
            out = jnp.where(cycle_of // 2 == n, full[:, n * LANES : (n + 1) * LANES], out)
        for f in range(fields):
            lensed_out[f, :, col * LANES : (col + 1) * LANES] = out[f * cycles_here : (f + 1) * cycles_here]


def turned(x, axis, n):
    return [lax.ppermute(x, axis, [(i, (i + k) % n) for i in range(n)]) for k in range(1, n)]


def local(alm, legendre, order_ids, cycle_number, src_band, src_block, weights):
    n_band, n_ord = lax.axis_size("band"), lax.axis_size("ord")
    parts, orders, _ = alm.shape
    fields = parts // 2
    cycles = legendre.shape[0]
    cycles_here = cycle_number.shape[0]
    blocks, blk, _ = weights.shape
    npix_here = blocks * blk // cycles_here
    band, slot = lax.axis_index("band"), lax.axis_index("ord")
    place = jnp.stack([band, slot]).astype(jnp.int32)
    width = (fields + 1) * 2 * orders
    smem = pl.BlockSpec(memory_space=pltpu.SMEM)
    vmem = pl.BlockSpec(memory_space=pltpu.VMEM)
    anywhere = pl.BlockSpec(memory_space=pl.ANY)
    part = pl.pallas_call(
        analysis,
        name="analysis",
        out_shape=jax.ShapeDtypeStruct((cycles, width), jnp.float32),
        in_specs=[smem, smem, vmem, anywhere, anywhere],
        out_specs=vmem,
        scratch_shapes=[
            pltpu.VMEM(legendre.shape, legendre.dtype),
            pltpu.VMEM(alm.shape, alm.dtype),
            pltpu.SemaphoreType.DMA((2, orders // GROUP)),
        ],
    )(place, cycle_number, order_ids[None], legendre, alm)
    if n_band <= 8:
        total = sum(turned(part, "band", n_band), part)
    else:
        total = lax.psum(part, "band")
    arrays = [total] + turned(total, "ord", n_ord)
    cols = npix_here // blk
    sky_map, lensed = pl.pallas_call(
        functools.partial(lens, n_ord, cycles_here, fields),
        name="lens",
        out_shape=(
            jax.ShapeDtypeStruct((fields, cycles_here, npix_here), jnp.bfloat16),
            jax.ShapeDtypeStruct((fields, cycles_here, npix_here), jnp.float32),
        ),
        in_specs=[smem, smem, smem] + [vmem] * n_ord + [anywhere],
        out_specs=(vmem, vmem),
        scratch_shapes=[
            pltpu.VMEM((cols * fields * cycles, blk), jnp.float32),
            pltpu.VMEM((2 * cols, 16, blk), jnp.float32),
            pltpu.VMEM(weights.shape, weights.dtype),
            pltpu.SemaphoreType.DMA,
        ],
    )(place, src_band[:, 0], src_block, *arrays, weights)
    return sky_map, lensed


def solution(mesh):
    placed = (
        P("sim", "ord", "band"),
        P(None, "ord", "band"),
        P("ord"),
        P("band"),
        P(("sim", "band", "ord"), None),
        P(("sim", "band", "ord")),
        P(("sim", "band", "ord"), None, None),
    )
    return jax.shard_map(
        local,
        mesh=mesh,
        in_specs=placed,
        out_specs=(P("sim", "band", "ord"), P("sim", "band", "ord")),
        check_vma=False,
    )
```

```python
import functools
import math

import jax
import jax.numpy as jnp
from jax import lax
from jax.experimental import pallas as pl
from jax.experimental.pallas import tpu as pltpu
from jax.sharding import PartitionSpec as P

LANES = 128
GROUP = 16
Q_LEN = 512
CHUNKS = 4
NT = (((1,), (1,)), ((), ()))
SINE = (6.2831851600887045, -41.34165503125142, 81.60100406374923, -76.54978209038376, 39.53670461908883)


def sin_turns(v):
    z = v * v
    total = SINE[-1]
    for term in SINE[-2::-1]:
        total = total * z + term
    return total * v


def wrap(u):
    return u - jnp.round(u)


def cos_turns(u):
    return sin_turns(0.25 - jnp.abs(u))


def split(x):
    high = x.astype(jnp.bfloat16)
    return high, (x - high.astype(jnp.float32)).astype(jnp.bfloat16)


def analysis(cycle_hbm, orders_hbm, legendre_hbm, alm_hbm, out_ref, legendre, alm, cycle_ref, orders_ref, sems):
    cycles, orders, _ = legendre.shape
    parts = alm.shape[0]
    half = parts // 2
    groups = orders // GROUP
    copies = []
    for g in range(groups):
        rows = pl.ds(g * GROUP, GROUP)
        copies.append(
            (
                pltpu.make_async_copy(alm_hbm.at[:, rows], alm.at[:, rows], sems.at[2 * g]),
                pltpu.make_async_copy(legendre_hbm.at[:, rows], legendre.at[:, rows], sems.at[2 * g + 1]),
            )
        )
    small = (
        pltpu.make_async_copy(cycle_hbm, cycle_ref, sems.at[2 * groups]),
        pltpu.make_async_copy(orders_hbm, orders_ref, sems.at[2 * groups + 1]),
    )
    for pair in copies[:1] + [small] + copies[1:]:
        for copy in pair:
            copy.start()

    for copy in small:
        copy.wait()
    band = lax.axis_index("band")
    cycles_here = cycle_ref.shape[0]
    row = lax.broadcasted_iota(jnp.int32, (cycles, LANES // 2), 0)
    parity = jnp.zeros((cycles, LANES // 2), jnp.float32)
    for i in range(cycles_here):
        odd = (cycle_ref[i] & 1).astype(jnp.float32)
        parity = jnp.where(row == band * cycles_here + i, odd, parity)
    ids = orders_ref[...].astype(jnp.float32) * jnp.where(band == 0, 1.0, 0.0)
    base = half * 2 * orders
    out_ref[:, base : base + orders] = jnp.broadcast_to(ids, (cycles, orders))
    out_ref[:, base + orders : base + 2 * orders] = parity

    width = parts * GROUP
    share = cycles // 2
    rows_of = lax.broadcasted_iota(jnp.int32, (share * GROUP, width), 0) % GROUP
    lane_of = lax.broadcasted_iota(jnp.int32, (share * GROUP, width), 1) % GROUP
    same = rows_of == lane_of
    sums = []
    for g in range(groups):
        for copy in copies[g]:
            copy.wait()
        rows = slice(g * GROUP, (g + 1) * GROUP)
        right = alm[:, rows, :].reshape(width, -1)
        both = []
        for h in range(2):
            left = legendre[h * share : (h + 1) * share, rows, :].reshape(share * GROUP, -1)
            full = lax.dot_general(left, right, NT, preferred_element_type=jnp.float32)
            full = jnp.where(same, full, 0.0)
            both.append(jnp.sum(full.reshape(share, GROUP, width), axis=1))
        sums.append(jnp.concatenate(both, axis=0))
    for f in range(half):
        pieces = [sums[g][:, c * GROUP : (c + 1) * GROUP] for c in (f, f + half) for g in range(groups)]
        out_ref[:, 2 * f * orders : 2 * (f + 1) * orders] = jnp.concatenate(pieces, axis=1)


def fetch(part_ref, weights_hbm, part_out, weights_ref, sem):
    copy = pltpu.make_async_copy(weights_hbm, weights_ref, sem)
    copy.start()
    part_out[...] = part_ref[...]
    copy.wait()


def synthesis(n_ord, fields, npix_here, arrays):
    slot = lax.axis_index("ord").astype(jnp.float32)
    cycles = arrays[0].shape[0]
    half = LANES // 2
    npix = npix_here * n_ord
    q_len = min(Q_LEN, npix_here)
    p_len = npix_here // q_len

    lane = lax.broadcasted_iota(jnp.int32, (cycles, LANES), 1)
    low = lane < half
    low_row = low[0:1]
    meta = [a[:, fields * LANES :] for a in arrays]
    ids = [jnp.where(low_row, m[0:1], pltpu.roll(m, half, 1)[0:1]) for m in meta]
    odd = jnp.where(low, pltpu.roll(meta[0], half, 1), meta[0]) > 0.5

    q_iota = lax.broadcasted_iota(jnp.int32, (LANES, q_len), 1).astype(jnp.float32) * (1.0 / npix)
    shift = jnp.where(lax.broadcasted_iota(jnp.int32, (LANES, q_len), 0) < half, 0.0, 0.25)
    table = []
    for m in ids:
        column = jnp.broadcast_to(m, (LANES, LANES)).T
        column = jnp.concatenate([column] * (q_len // LANES), axis=1)
        table.append(split(cos_turns(wrap(column * q_iota - shift))))
    table_high, table_low = (jnp.concatenate(v, axis=0) for v in zip(*table))

    p_iota = lax.broadcasted_iota(jnp.int32, (p_len, LANES), 0).astype(jnp.float32) * (q_len / npix)
    low_p = lax.broadcasted_iota(jnp.int32, (p_len, LANES), 1) < half
    columns = []
    for a, m in zip(arrays, ids):
        factor = jnp.where(m == 0.0, 1.0, 2.0)
        start = wrap(m * (slot * (1.0 / n_ord)))
        even_turn = wrap(wrap(m * p_iota) + start)
        odd_turn = wrap(even_turn + wrap(m * (0.5 / npix)))
        terms = []
        for turn in (even_turn, odd_turn):
            cosine = cos_turns(turn) * factor
            sine = cos_turns(wrap(turn - 0.25)) * factor
            terms.append((jnp.where(low_p, cosine, -cosine), -sine))
        x = [a[:, f * LANES : (f + 1) * LANES] for f in range(fields)]
        crossed_x = [pltpu.roll(v, half, 1) for v in x]
        rows = []
        for p in range(p_len):
            straight = jnp.where(odd, terms[1][0][p : p + 1], terms[0][0][p : p + 1])
            crossed = jnp.where(odd, terms[1][1][p : p + 1], terms[0][1][p : p + 1])
            rows += [x[f] * straight + crossed_x[f] * crossed for f in range(fields)]
        columns.append(split(jnp.concatenate(rows, axis=0)))
    high, low_part = (jnp.concatenate(v, axis=1) for v in zip(*columns))
    dot = functools.partial(jnp.dot, preferred_element_type=jnp.float32)
    return dot(high, table_high) + (dot(low_part, table_high) + dot(high, table_low))


def near(n_ord, fields, npix_here, *refs):
    refs[-1][...] = synthesis(n_ord, fields, npix_here, [r[...] for r in refs[:-1]])


def lens(n_ord, cycles_here, fields, src_band_ref, src_block_ref, *refs):
    arrays = refs[: n_ord // 2]
    near_ref, weights, sky_hbm, lensed_hbm, sky, stage, sky_out, lensed_out, sems = refs[n_ord // 2 :]
    band = lax.axis_index("band")
    cycles = arrays[0].shape[0]
    npix_here = sky_out.shape[2]
    cols = npix_here // LANES
    q_len = near_ref.shape[1]
    p_len = npix_here // q_len
    rows_col = fields * cycles

    pixels = near_ref[...] + synthesis(n_ord, fields, npix_here, [r[...] for r in arrays])
    pixels = pixels.astype(jnp.bfloat16).astype(jnp.float32)
    for p in range(p_len):
        for j in range(q_len // LANES):
            col = p * (q_len // LANES) + j
            sky[col * rows_col : (col + 1) * rows_col, :] = pixels[
                p * rows_col : (p + 1) * rows_col, j * LANES : (j + 1) * LANES
            ]

    first = pl.multiple_of(band * cycles_here, cycles_here)
    for col in range(cols):
        for f in range(fields):
            own = sky[pl.ds(col * rows_col + f * cycles + first, cycles_here), :]
            sky_out[f, :, col * LANES : (col + 1) * LANES] = own.astype(jnp.bfloat16)
    copies = [pltpu.make_async_copy(sky_out, sky_hbm, sems.at[0])]
    copies[0].start()

    shift_bits = cols.bit_length() - 1
    stage[...] = jnp.zeros_like(stage)
    for col in range(cols):
        for c in range(cycles_here):
            k = c * cols + col
            block = src_block_ref[k]
            cycle = src_band_ref[k] * cycles_here + lax.shift_right_logical(block, shift_bits)
            begin = (block & (cols - 1)) * rows_col + cycle
            source = sky[pl.ds(begin, fields, stride=cycles), :]
            stage[2 * col + c % 2, pl.ds(c, fields, stride=cycles_here), :] = source

    rows = stage.shape[1]
    cycle_of = lax.broadcasted_iota(jnp.int32, (rows, LANES), 0) % cycles_here
    chunk = cols // CHUNKS
    for col in range(cols):
        left = jnp.concatenate([stage[2 * col], stage[2 * col + 1]], axis=1).astype(jnp.bfloat16)
        right = jnp.concatenate(
            [
                jnp.concatenate([weights[c * cols + col], weights[(c + 1) * cols + col]], axis=1)
                for c in range(0, cycles_here, 2)
            ],
            axis=0,
        )
        full = lax.dot_general(left, right, NT, preferred_element_type=jnp.float32)
        out = full[:, 0:LANES]
        for n in range(1, cycles_here // 2):
            out = jnp.where(cycle_of // 2 == n, full[:, n * LANES : (n + 1) * LANES], out)
        for f in range(fields):
            lensed_out[f, :, col * LANES : (col + 1) * LANES] = out[f * cycles_here : (f + 1) * cycles_here]
        if (col + 1) % chunk == 0:
            lanes = pl.ds((col + 1 - chunk) * LANES, chunk * LANES)
            copies.append(
                pltpu.make_async_copy(
                    lensed_out.at[:, :, lanes], lensed_hbm.at[:, :, lanes], sems.at[(col + 1) // chunk]
                )
            )
            copies[-1].start()
    for copy in copies:
        copy.wait()


def crossed(x, axis, n):
    return [lax.ppermute(x, axis, [(i, i ^ k) for i in range(n)]) for k in range(1, n)]


def local(alm, legendre, order_ids, cycle_number, src_band, src_block, weights):
    n_band, n_ord = lax.axis_size("band"), lax.axis_size("ord")
    parts, orders, _ = alm.shape
    fields = parts // 2
    cycles = legendre.shape[0]
    cycles_here = cycle_number.shape[0]
    blocks, blk, _ = weights.shape
    npix_here = blocks * blk // cycles_here
    width = (fields + 1) * 2 * orders
    cols = npix_here // blk
    q_len = min(Q_LEN, npix_here)
    smem = pl.BlockSpec(memory_space=pltpu.SMEM)
    vmem = pl.BlockSpec(memory_space=pltpu.VMEM)
    hbm = pl.BlockSpec(memory_space=pltpu.HBM)

    def far(*arrays):
        return [pltpu.with_memory_space_constraint(v, pltpu.HBM) for v in arrays]

    part = pl.pallas_call(
        analysis,
        name="analysis",
        out_shape=pltpu.VMEM((cycles, width), jnp.float32),
        in_specs=[hbm] * 4,
        out_specs=vmem,
        scratch_shapes=[
            pltpu.VMEM(legendre.shape, legendre.dtype),
            pltpu.VMEM(alm.shape, alm.dtype),
            pltpu.SMEM(cycle_number.shape, jnp.int32),
            pltpu.VMEM((1, orders), jnp.int32),
            pltpu.SemaphoreType.DMA((2 * (orders // GROUP) + 2,)),
        ],
        compiler_params=pltpu.CompilerParams(vmem_limit_bytes=16 << 20),
        cost_estimate=pl.CostEstimate(flops=2 << 30, bytes_accessed=6 << 20, transcendentals=0),
    )(*far(cycle_number, order_ids[None], legendre, alm))
    own, weights = pl.pallas_call(
        fetch,
        name="fetch",
        out_shape=(pltpu.VMEM(part.shape, part.dtype), pltpu.VMEM(weights.shape, weights.dtype)),
        in_specs=[vmem, hbm],
        out_specs=(vmem, vmem),
        scratch_shapes=[pltpu.SemaphoreType.DMA],
        compiler_params=pltpu.CompilerParams(vmem_limit_bytes=8 << 20),
        cost_estimate=pl.CostEstimate(flops=1 << 30, bytes_accessed=6 << 20, transcendentals=0),
    )(part, *far(weights))
    if n_band <= 8:
        total = sum(crossed(part, "band", n_band), own)
    else:
        total = lax.psum(own, "band")
    arrays = [total] + crossed(total, "ord", n_ord)
    first = pl.pallas_call(
        functools.partial(near, n_ord, fields, npix_here),
        name="near",
        out_shape=pltpu.VMEM((npix_here // q_len * fields * cycles, q_len), jnp.float32),
        in_specs=[vmem] * (n_ord // 2),
        out_specs=vmem,
        compiler_params=pltpu.CompilerParams(vmem_limit_bytes=16 << 20),
        cost_estimate=pl.CostEstimate(flops=1 << 30, bytes_accessed=1 << 20, transcendentals=0),
    )(*arrays[: n_ord // 2])
    pixels = (fields, cycles_here, npix_here)
    return pl.pallas_call(
        functools.partial(lens, n_ord, cycles_here, fields),
        name="lens",
        out_shape=(jax.ShapeDtypeStruct(pixels, jnp.bfloat16), jax.ShapeDtypeStruct(pixels, jnp.float32)),
        in_specs=[smem, smem] + [vmem] * (n_ord // 2 + 2),
        out_specs=(hbm, hbm),
        scratch_shapes=[
            pltpu.VMEM((cols * fields * cycles, blk), jnp.float32),
            pltpu.VMEM((2 * cols, 16, blk), jnp.float32),
            pltpu.VMEM(pixels, jnp.bfloat16),
            pltpu.VMEM(pixels, jnp.float32),
            pltpu.SemaphoreType.DMA((CHUNKS + 1,)),
        ],
        compiler_params=pltpu.CompilerParams(vmem_limit_bytes=32 << 20),
    )(src_band[:, 0], src_block, *arrays[n_ord // 2 :], first, weights)


def solution(mesh):
    placed = (
        P("sim", "ord", "band"),
        P(None, "ord", "band"),
        P("ord"),
        P("band"),
        P(("sim", "band", "ord"), None),
        P(("sim", "band", "ord")),
        P(("sim", "band", "ord"), None, None),
    )
    return jax.shard_map(
        local,
        mesh=mesh,
        in_specs=placed,
        out_specs=(P("sim", "band", "ord"), P("sim", "band", "ord")),
        check_vma=False,
    )
```

```python
import functools

import jax
import jax.numpy as jnp
from jax import lax
from jax.experimental import pallas as pl
from jax.experimental.pallas import tpu as pltpu
from jax.sharding import PartitionSpec as P


LANES = 128
GROUP = 16
Q_LEN = 512
CHUNKS = 4
UNROLL = 8
NT = (((1,), (1,)), ((), ()))
SINE = (6.2831851600887045, -41.34165503125142, 81.60100406374923, -76.54978209038376, 39.53670461908883)


def sin_turns(v):
    z = v * v
    total = SINE[-1]
    for term in SINE[-2::-1]:
        total = total * z + term
    return total * v


def wrap(u):
    return u - jnp.round(u)


def cos_turns(u):
    return sin_turns(0.25 - jnp.abs(u))


def split(x):
    high = x.astype(jnp.bfloat16)
    return high, (x - high.astype(jnp.float32)).astype(jnp.bfloat16)


def analysis(cycle_hbm, orders_hbm, legendre_hbm, alm_hbm, out_ref, legendre, alm, cycle_ref, orders_ref, sems):
    cycles, orders, _ = legendre.shape
    parts = alm.shape[0]
    half = parts // 2
    groups = orders // GROUP
    copies = []
    for g in range(groups):
        rows = pl.ds(g * GROUP, GROUP)
        copies.append(
            (
                pltpu.make_async_copy(alm_hbm.at[:, rows], alm.at[:, rows], sems.at[2 * g]),
                pltpu.make_async_copy(legendre_hbm.at[:, rows], legendre.at[:, rows], sems.at[2 * g + 1]),
            )
        )
    small = (
        pltpu.make_async_copy(cycle_hbm, cycle_ref, sems.at[2 * groups]),
        pltpu.make_async_copy(orders_hbm, orders_ref, sems.at[2 * groups + 1]),
    )
    for pair in copies[:1] + [small] + copies[1:]:
        for copy in pair:
            copy.start()

    for copy in small:
        copy.wait()
    band = lax.axis_index("band")
    cycles_here = cycle_ref.shape[0]
    row = lax.broadcasted_iota(jnp.int32, (cycles, LANES // 2), 0)
    parity = jnp.zeros((cycles, LANES // 2), jnp.float32)
    for i in range(cycles_here):
        odd = (cycle_ref[i] & 1).astype(jnp.float32)
        parity = jnp.where(row == band * cycles_here + i, odd, parity)
    ids = orders_ref[...].astype(jnp.float32) * jnp.where(band == 0, 1.0, 0.0)
    base = half * 2 * orders
    out_ref[:, base : base + orders] = jnp.broadcast_to(ids, (cycles, orders))
    out_ref[:, base + orders : base + 2 * orders] = parity

    width = parts * GROUP
    share = cycles // 2
    rows_of = lax.broadcasted_iota(jnp.int32, (share * GROUP, width), 0) % GROUP
    lane_of = lax.broadcasted_iota(jnp.int32, (share * GROUP, width), 1) % GROUP
    same = rows_of == lane_of
    sums = []
    for g in range(groups):
        for copy in copies[g]:
            copy.wait()
        rows = slice(g * GROUP, (g + 1) * GROUP)
        right = alm[:, rows, :].reshape(width, -1)
        both = []
        for h in range(2):
            left = legendre[h * share : (h + 1) * share, rows, :].reshape(share * GROUP, -1)
            full = lax.dot_general(left, right, NT, preferred_element_type=jnp.float32)
            full = jnp.where(same, full, 0.0)
            both.append(jnp.sum(full.reshape(share, GROUP, width), axis=1))
        sums.append(jnp.concatenate(both, axis=0))
    for f in range(half):
        pieces = [sums[g][:, c * GROUP : (c + 1) * GROUP] for c in (f, f + half) for g in range(groups)]
        out_ref[:, 2 * f * orders : 2 * (f + 1) * orders] = jnp.concatenate(pieces, axis=1)


def fetch(part_ref, weights_hbm, part_out, weights_ref, stage, sems):
    count = weights_ref.shape[0] // CHUNKS
    copies = [
        pltpu.make_async_copy(
            weights_hbm.at[pl.ds(i * count, count)], stage.at[pl.ds(i * count, count)], sems.at[i]
        )
        for i in range(CHUNKS)
    ]
    for copy in copies:
        copy.start()
    part_out[...] = part_ref[...]
    for i, copy in enumerate(copies):
        copy.wait()

        @pl.loop(0, count, step=UNROLL)
        def _(k):
            for j in range(UNROLL):
                weights_ref[i * count + k + j] = stage[i * count + k + j].T


def synthesis(n_ord, fields, npix_here, arrays):
    slot = lax.axis_index("ord").astype(jnp.float32)
    cycles = arrays[0].shape[0]
    half = LANES // 2
    npix = npix_here * n_ord
    q_len = min(Q_LEN, npix_here)
    p_len = npix_here // q_len

    lane = lax.broadcasted_iota(jnp.int32, (cycles, LANES), 1)
    low = lane < half
    low_row = low[0:1]
    meta = [a[:, fields * LANES :] for a in arrays]
    ids = [jnp.where(low_row, m[0:1], pltpu.roll(m, half, 1)[0:1]) for m in meta]
    odd = jnp.where(low, pltpu.roll(meta[0], half, 1), meta[0]) > 0.5

    q_iota = lax.broadcasted_iota(jnp.int32, (LANES, q_len), 1).astype(jnp.float32) * (1.0 / npix)
    shift = jnp.where(lax.broadcasted_iota(jnp.int32, (LANES, q_len), 0) < half, 0.0, 0.25)
    table = []
    for m in ids:
        column = jnp.broadcast_to(m, (LANES, LANES)).T
        column = jnp.concatenate([column] * (q_len // LANES), axis=1)
        table.append(split(cos_turns(wrap(column * q_iota - shift))))
    table_high, table_low = (jnp.concatenate(v, axis=0) for v in zip(*table))

    p_iota = lax.broadcasted_iota(jnp.int32, (p_len, LANES), 0).astype(jnp.float32) * (q_len / npix)
    low_p = lax.broadcasted_iota(jnp.int32, (p_len, LANES), 1) < half
    columns = []
    for a, m in zip(arrays, ids):
        factor = jnp.where(m == 0.0, 1.0, 2.0)
        start = wrap(m * (slot * (1.0 / n_ord)))
        even_turn = wrap(wrap(m * p_iota) + start)
        odd_turn = wrap(even_turn + wrap(m * (0.5 / npix)))
        terms = []
        for turn in (even_turn, odd_turn):
            cosine = cos_turns(turn) * factor
            sine = cos_turns(wrap(turn - 0.25)) * factor
            terms.append((jnp.where(low_p, cosine, -cosine), -sine))
        x = [a[:, f * LANES : (f + 1) * LANES] for f in range(fields)]
        crossed_x = [pltpu.roll(v, half, 1) for v in x]
        rows = []
        for p in range(p_len):
            straight = jnp.where(odd, terms[1][0][p : p + 1], terms[0][0][p : p + 1])
            crossed = jnp.where(odd, terms[1][1][p : p + 1], terms[0][1][p : p + 1])
            rows += [x[f] * straight + crossed_x[f] * crossed for f in range(fields)]
        columns.append(split(jnp.concatenate(rows, axis=0)))
    high, low_part = (jnp.concatenate(v, axis=1) for v in zip(*columns))
    dot = functools.partial(jnp.dot, preferred_element_type=jnp.float32)
    if len(arrays) == 1:
        both = jnp.concatenate([high, low_part], axis=1)
        return dot(both, jnp.concatenate([table_high] * 2, axis=0)) + dot(high, table_low)
    return dot(high, table_high) + (dot(low_part, table_high) + dot(high, table_low))


def near(n_ord, fields, npix_here, *refs):
    refs[-1][...] = synthesis(n_ord, fields, npix_here, [r[...] for r in refs[:-1]])


def next_near(n_ord, fields, npix_here, array_ref, before_ref, out_ref):
    out_ref[...] = before_ref[...] + synthesis(n_ord, fields, npix_here, [array_ref[...]])


def lens(n_ord, cycles_here, fields, src_band_ref, src_block_ref, *refs):
    last = n_ord // 2 - 1
    arrays = refs[:last]
    near_ref, weights, sky_hbm, lensed_hbm, sky, stage, sky_out, lensed_out, sems = refs[last:]
    band = lax.axis_index("band")
    cycles = arrays[0].shape[0]
    npix_here = sky_out.shape[2]
    cols = npix_here // LANES
    q_len = near_ref.shape[1]
    p_len = npix_here // q_len
    rows_col = fields * cycles

    pixels = near_ref[...] + synthesis(n_ord, fields, npix_here, [r[...] for r in arrays])
    pixels = pixels.astype(jnp.bfloat16).astype(jnp.float32)
    for p in range(p_len):
        for j in range(q_len // LANES):
            col = p * (q_len // LANES) + j
            sky[col * rows_col : (col + 1) * rows_col, :] = pixels[
                p * rows_col : (p + 1) * rows_col, j * LANES : (j + 1) * LANES
            ]

    first = pl.multiple_of(band * cycles_here, cycles_here)
    for col in range(cols):
        for f in range(fields):
            own = sky[pl.ds(col * rows_col + f * cycles + first, cycles_here), :]
            sky_out[f, :, col * LANES : (col + 1) * LANES] = own.astype(jnp.bfloat16)
    copies = [pltpu.make_async_copy(sky_out, sky_hbm, sems.at[0])]
    copies[0].start()

    shift_bits = cols.bit_length() - 1
    stage[...] = jnp.zeros_like(stage)
    for col in range(cols):
        for c in range(cycles_here):
            k = c * cols + col
            block = src_block_ref[k]
            cycle = src_band_ref[k] * cycles_here + lax.shift_right_logical(block, shift_bits)
            begin = (block & (cols - 1)) * rows_col + cycle
            source = sky[pl.ds(begin, fields, stride=cycles), :]
            stage[2 * col + c % 2, pl.ds(c, fields, stride=cycles_here), :] = source

    rows = stage.shape[1]
    cycle_of = lax.broadcasted_iota(jnp.int32, (rows, LANES), 0) % cycles_here
    chunk = cols // CHUNKS
    for col in range(cols):
        left = jnp.concatenate([stage[2 * col], stage[2 * col + 1]], axis=1).astype(jnp.bfloat16)
        right = jnp.concatenate(
            [
                jnp.concatenate([weights[c * cols + col] for c in range(n, cycles_here, 2)], axis=1)
                for n in range(2)
            ],
            axis=0,
        )
        full = jnp.dot(left, right, preferred_element_type=jnp.float32)
        out = full[:, 0:LANES]
        for n in range(1, cycles_here // 2):
            out = jnp.where(cycle_of // 2 == n, full[:, n * LANES : (n + 1) * LANES], out)
        for f in range(fields):
            lensed_out[f, :, col * LANES : (col + 1) * LANES] = out[f * cycles_here : (f + 1) * cycles_here]
        if (col + 1) % chunk == 0:
            lanes = pl.ds((col + 1 - chunk) * LANES, chunk * LANES)
            copies.append(
                pltpu.make_async_copy(
                    lensed_out.at[:, :, lanes], lensed_hbm.at[:, :, lanes], sems.at[(col + 1) // chunk]
                )
            )
            copies[-1].start()
    for copy in copies:
        copy.wait()


def crossed(x, axis, n):
    out = []
    for k in range(1, n):
        out.append(lax.ppermute(x, axis, [(i, i ^ k) for i in range(n)]))
    return out


def local(alm, legendre, order_ids, cycle_number, src_band, src_block, weights):
    n_band, n_ord = lax.axis_size("band"), lax.axis_size("ord")
    parts, orders, _ = alm.shape
    fields = parts // 2
    cycles = legendre.shape[0]
    cycles_here = cycle_number.shape[0]
    blocks, blk, _ = weights.shape
    npix_here = blocks * blk // cycles_here
    width = (fields + 1) * 2 * orders
    cols = npix_here // blk
    q_len = min(Q_LEN, npix_here)
    smem = pl.BlockSpec(memory_space=pltpu.SMEM)
    vmem = pl.BlockSpec(memory_space=pltpu.VMEM)
    hbm = pl.BlockSpec(memory_space=pltpu.HBM)

    def far(*arrays):
        return [pltpu.with_memory_space_constraint(v, pltpu.HBM) for v in arrays]

    part = pl.pallas_call(
        analysis,
        name="analysis",
        out_shape=pltpu.VMEM((cycles, width), jnp.float32),
        in_specs=[hbm] * 4,
        out_specs=vmem,
        scratch_shapes=[
            pltpu.VMEM(legendre.shape, legendre.dtype),
            pltpu.VMEM(alm.shape, alm.dtype),
            pltpu.SMEM(cycle_number.shape, jnp.int32),
            pltpu.VMEM((1, orders), jnp.int32),
            pltpu.SemaphoreType.DMA((2 * (orders // GROUP) + 2,)),
        ],
        compiler_params=pltpu.CompilerParams(vmem_limit_bytes=16 << 20),
        cost_estimate=pl.CostEstimate(flops=2 << 30, bytes_accessed=6 << 20, transcendentals=0),
    )(*far(cycle_number, order_ids[None], legendre, alm))
    own, weights = pl.pallas_call(
        fetch,
        name="fetch",
        out_shape=(pltpu.VMEM(part.shape, part.dtype), pltpu.VMEM(weights.shape, weights.dtype)),
        in_specs=[vmem, hbm],
        out_specs=(vmem, vmem),
        scratch_shapes=[pltpu.VMEM(weights.shape, weights.dtype), pltpu.SemaphoreType.DMA((CHUNKS,))],
        compiler_params=pltpu.CompilerParams(vmem_limit_bytes=16 << 20),
        cost_estimate=pl.CostEstimate(flops=1 << 30, bytes_accessed=6 << 20, transcendentals=0),
    )(part, *far(weights))
    if n_band <= 8:
        total = sum(crossed(part, "band", n_band), own)
    else:
        total = lax.psum(own, "band")

    def swap(x, k):
        return lax.ppermute(x, "ord", [(i, i ^ k) for i in range(n_ord)])

    half = n_ord // 2
    here = [total] + [swap(total, k) for k in range(1, half)]
    there = swap(total, half)
    rest = [swap(there, k) for k in range(1, half)]
    synth = dict(
        out_shape=pltpu.VMEM((npix_here // q_len * fields * cycles, q_len), jnp.float32),
        out_specs=vmem,
        compiler_params=pltpu.CompilerParams(vmem_limit_bytes=16 << 20),
        cost_estimate=pl.CostEstimate(flops=1 << 30, bytes_accessed=1 << 20, transcendentals=0),
    )
    sums = pl.pallas_call(
        functools.partial(near, n_ord, fields, npix_here), name="near", in_specs=[vmem] * half, **synth
    )(*here)
    sums = pl.pallas_call(
        functools.partial(next_near, n_ord, fields, npix_here), name="next_near", in_specs=[vmem] * 2, **synth
    )(there, sums)
    pixels = (fields, cycles_here, npix_here)
    return pl.pallas_call(
        functools.partial(lens, n_ord, cycles_here, fields),
        name="lens",
        out_shape=(jax.ShapeDtypeStruct(pixels, jnp.bfloat16), jax.ShapeDtypeStruct(pixels, jnp.float32)),
        in_specs=[smem, smem] + [vmem] * (half + 1),
        out_specs=(hbm, hbm),
        scratch_shapes=[
            pltpu.VMEM((cols * fields * cycles, blk), jnp.float32),
            pltpu.VMEM((2 * cols, 16, blk), jnp.float32),
            pltpu.VMEM(pixels, jnp.bfloat16),
            pltpu.VMEM(pixels, jnp.float32),
            pltpu.SemaphoreType.DMA((CHUNKS + 1,)),
        ],
        compiler_params=pltpu.CompilerParams(vmem_limit_bytes=32 << 20),
    )(src_band[:, 0], src_block, *rest, sums, weights)


def solution(mesh):
    placed = (
        P("sim", "ord", "band"),
        P(None, "ord", "band"),
        P("ord"),
        P("band"),
        P(("sim", "band", "ord"), None),
        P(("sim", "band", "ord")),
        P(("sim", "band", "ord"), None, None),
    )
    return jax.shard_map(
        local,
        mesh=mesh,
        in_specs=placed,
        out_specs=(P("sim", "band", "ord"), P("sim", "band", "ord")),
        check_vma=False,
    )
```

```python
import functools

import jax
import jax.numpy as jnp
from jax import lax
from jax.experimental import pallas as pl
from jax.experimental.pallas import tpu as pltpu
from jax.sharding import PartitionSpec as P


LANES = 128
GROUP = 16
Q_LEN = 512
CHUNKS = 4
UNROLL = 8
META = 8
NT = (((1,), (1,)), ((), ()))
SINE = (6.2831851600887045, -41.34165503125142, 81.60100406374923, -76.54978209038376, 39.53670461908883)


def sin_turns(v):
    z = v * v
    total = SINE[-1]
    for term in SINE[-2::-1]:
        total = total * z + term
    return total * v


def wrap(u):
    return u - jnp.round(u)


def cos_turns(u):
    return sin_turns(0.25 - jnp.abs(u))


def split(x):
    high = x.astype(jnp.bfloat16)
    return high, (x - high.astype(jnp.float32)).astype(jnp.bfloat16)


def analysis(cycle_hbm, orders_hbm, legendre_hbm, alm_hbm, out_ref, legendre, alm, cycle_ref, orders_ref, sems):
    cycles, orders, _ = legendre.shape
    parts = alm.shape[0]
    half = parts // 2
    groups = orders // GROUP
    copies = []
    for g in range(groups):
        rows = pl.ds(g * GROUP, GROUP)
        copies.append(
            (
                pltpu.make_async_copy(alm_hbm.at[:, rows], alm.at[:, rows], sems.at[2 * g]),
                pltpu.make_async_copy(legendre_hbm.at[:, rows], legendre.at[:, rows], sems.at[2 * g + 1]),
            )
        )
    small = (
        pltpu.make_async_copy(cycle_hbm, cycle_ref, sems.at[2 * groups]),
        pltpu.make_async_copy(orders_hbm, orders_ref, sems.at[2 * groups + 1]),
    )
    for pair in copies[:1] + [small] + copies[1:]:
        for copy in pair:
            copy.start()

    for copy in small:
        copy.wait()
    band = lax.axis_index("band")
    cycles_here = cycle_ref.shape[0]
    lane = lax.broadcasted_iota(jnp.int32, (1, LANES), 1)
    parity = jnp.zeros((1, LANES), jnp.float32)
    for i in range(cycles_here):
        odd = (cycle_ref[i] & 1).astype(jnp.float32)
        parity = jnp.where(lane == band * cycles_here + i, odd, parity)
    ids = orders_ref[...].astype(jnp.float32) * jnp.where(band == 0, 1.0, 0.0)
    base = half * cycles
    out_ref[base : base + 1, :] = jnp.concatenate([ids, ids], axis=1)
    out_ref[base + 1 : base + 2, :] = parity
    out_ref[base + 2 :, :] = jnp.zeros((META - 2, LANES), jnp.float32)

    width = parts * GROUP
    share = cycles // 2
    rows_of = lax.broadcasted_iota(jnp.int32, (share * GROUP, width), 0) % GROUP
    lane_of = lax.broadcasted_iota(jnp.int32, (share * GROUP, width), 1) % GROUP
    same = rows_of == lane_of
    sums = []
    for g in range(groups):
        for copy in copies[g]:
            copy.wait()
        rows = slice(g * GROUP, (g + 1) * GROUP)
        right = alm[:, rows, :].reshape(width, -1)
        both = []
        for h in range(2):
            left = legendre[h * share : (h + 1) * share, rows, :].reshape(share * GROUP, -1)
            full = lax.dot_general(left, right, NT, preferred_element_type=jnp.float32)
            full = jnp.where(same, full, 0.0)
            both.append(jnp.sum(full.reshape(share, GROUP, width), axis=1))
        sums.append(jnp.concatenate(both, axis=0))
    for f in range(half):
        pieces = [sums[g][:, c * GROUP : (c + 1) * GROUP] for c in (f, f + half) for g in range(groups)]
        out_ref[f * cycles : (f + 1) * cycles, :] = jnp.concatenate(pieces, axis=1)


def fetch(cycles_here, rows_col, cols, part_ref, src_band_ref, src_block_ref, weights_hbm, part_out, places_ref, weights_ref, stage, sems):
    count = weights_ref.shape[0] // CHUNKS
    copies = [
        pltpu.make_async_copy(
            weights_hbm.at[pl.ds(i * count, count)], stage.at[pl.ds(i * count, count)], sems.at[i]
        )
        for i in range(CHUNKS)
    ]
    for copy in copies:
        copy.start()
    part_out[...] = part_ref[...]
    block = src_block_ref[...]
    cycle = src_band_ref[...] * cycles_here + lax.shift_right_logical(block, cols.bit_length() - 1)
    places_ref[...] = (block & (cols - 1)) * rows_col + cycle
    for i, copy in enumerate(copies):
        copy.wait()

        @pl.loop(0, count, step=UNROLL)
        def _(k):
            for j in range(UNROLL):
                weights_ref[i * count + k + j] = stage[i * count + k + j].T


def synthesis(n_ord, fields, npix_here, arrays):
    slot = lax.axis_index("ord").astype(jnp.float32)
    base = arrays[0].shape[0] - META
    cycles = base // fields
    half = LANES // 2
    npix = npix_here * n_ord
    q_len = min(Q_LEN, npix_here)
    p_len = npix_here // q_len

    ids = [a[base : base + 1] for a in arrays]
    odd = jnp.broadcast_to(arrays[0][base + 1 : base + 2], (LANES, LANES)).T[:cycles] > 0.5

    q_iota = lax.broadcasted_iota(jnp.int32, (LANES, q_len), 1).astype(jnp.float32) * (1.0 / npix)
    shift = jnp.where(lax.broadcasted_iota(jnp.int32, (LANES, q_len), 0) < half, 0.0, 0.25)
    table = []
    for m in ids:
        column = jnp.broadcast_to(m, (LANES, LANES)).T
        column = jnp.concatenate([column] * (q_len // LANES), axis=1)
        table.append(split(cos_turns(wrap(column * q_iota - shift))))
    table_high, table_low = (jnp.concatenate(v, axis=0) for v in zip(*table))

    p_iota = lax.broadcasted_iota(jnp.int32, (p_len, LANES), 0).astype(jnp.float32) * (q_len / npix)
    low_p = lax.broadcasted_iota(jnp.int32, (p_len, LANES), 1) < half
    columns = []
    for a, m in zip(arrays, ids):
        factor = jnp.where(m == 0.0, 1.0, 2.0)
        start = wrap(m * (slot * (1.0 / n_ord)))
        even_turn = wrap(wrap(m * p_iota) + start)
        odd_turn = wrap(even_turn + wrap(m * (0.5 / npix)))
        terms = []
        for turn in (even_turn, odd_turn):
            cosine = cos_turns(turn) * factor
            sine = cos_turns(wrap(turn - 0.25)) * factor
            terms.append((jnp.where(low_p, cosine, -cosine), -sine))
        x = [a[f * cycles : (f + 1) * cycles] for f in range(fields)]
        crossed_x = [pltpu.roll(v, half, 1) for v in x]
        rows = []
        for p in range(p_len):
            straight = jnp.where(odd, terms[1][0][p : p + 1], terms[0][0][p : p + 1])
            crossed = jnp.where(odd, terms[1][1][p : p + 1], terms[0][1][p : p + 1])
            rows += [x[f] * straight + crossed_x[f] * crossed for f in range(fields)]
        columns.append(split(jnp.concatenate(rows, axis=0)))
    high, low_part = (jnp.concatenate(v, axis=1) for v in zip(*columns))
    dot = functools.partial(jnp.dot, preferred_element_type=jnp.float32)
    if len(arrays) == 1:
        both = jnp.concatenate([high, low_part], axis=1)
        return dot(both, jnp.concatenate([table_high] * 2, axis=0)) + dot(high, table_low)
    return dot(high, table_high) + (dot(low_part, table_high) + dot(high, table_low))


def near(n_ord, fields, npix_here, *refs):
    refs[-1][...] = synthesis(n_ord, fields, npix_here, [r[...] for r in refs[:-1]])


def next_near(n_ord, fields, npix_here, array_ref, before_ref, out_ref):
    out_ref[...] = before_ref[...] + synthesis(n_ord, fields, npix_here, [array_ref[...]])


def lens(n_ord, cycles_here, fields, places_vmem, *refs):
    last = n_ord // 2 - 1
    arrays = refs[:last]
    near_ref, weights, sky_hbm, lensed_hbm, sky, stage, sky_out, lensed_out, places, sems = refs[last:]
    listing = pltpu.make_async_copy(places_vmem, places, sems.at[CHUNKS + 1])
    listing.start()
    band = lax.axis_index("band")
    cycles = (arrays[0].shape[0] - META) // fields
    npix_here = sky_out.shape[2]
    cols = npix_here // LANES
    q_len = near_ref.shape[1]
    p_len = npix_here // q_len
    rows_col = fields * cycles

    pixels = near_ref[...] + synthesis(n_ord, fields, npix_here, [r[...] for r in arrays])
    pixels = pixels.astype(jnp.bfloat16).astype(jnp.float32)
    for p in range(p_len):
        for j in range(q_len // LANES):
            col = p * (q_len // LANES) + j
            sky[col * rows_col : (col + 1) * rows_col, :] = pixels[
                p * rows_col : (p + 1) * rows_col, j * LANES : (j + 1) * LANES
            ]

    first = pl.multiple_of(band * cycles_here, cycles_here)
    for col in range(cols):
        for f in range(fields):
            own = sky[pl.ds(col * rows_col + f * cycles + first, cycles_here), :]
            sky_out[f, :, col * LANES : (col + 1) * LANES] = own.astype(jnp.bfloat16)
    copies = [pltpu.make_async_copy(sky_out, sky_hbm, sems.at[0])]
    copies[0].start()

    listing.wait()
    stage[...] = jnp.zeros_like(stage)
    for col in range(cols):
        for c in range(cycles_here):
            source = sky[pl.ds(places[0, c * cols + col], fields, stride=cycles), :]
            stage[2 * col + c % 2, pl.ds(c, fields, stride=cycles_here), :] = source

    rows = stage.shape[1]
    cycle_of = lax.broadcasted_iota(jnp.int32, (rows, LANES), 0) % cycles_here
    chunk = cols // CHUNKS
    for col in range(cols):
        left = jnp.concatenate([stage[2 * col], stage[2 * col + 1]], axis=1).astype(jnp.bfloat16)
        right = jnp.concatenate(
            [
                jnp.concatenate([weights[c * cols + col] for c in range(n, cycles_here, 2)], axis=1)
                for n in range(2)
            ],
            axis=0,
        )
        full = jnp.dot(left, right, preferred_element_type=jnp.float32)
        out = full[:, 0:LANES]
        for n in range(1, cycles_here // 2):
            out = jnp.where(cycle_of // 2 == n, full[:, n * LANES : (n + 1) * LANES], out)
        for f in range(fields):
            lensed_out[f, :, col * LANES : (col + 1) * LANES] = out[f * cycles_here : (f + 1) * cycles_here]
        if (col + 1) % chunk == 0:
            lanes = pl.ds((col + 1 - chunk) * LANES, chunk * LANES)
            copies.append(
                pltpu.make_async_copy(
                    lensed_out.at[:, :, lanes], lensed_hbm.at[:, :, lanes], sems.at[(col + 1) // chunk]
                )
            )
            copies[-1].start()
    for copy in copies:
        copy.wait()


def crossed(x, axis, n):
    out = []
    for k in range(1, n):
        out.append(lax.ppermute(x, axis, [(i, i ^ k) for i in range(n)]))
    return out


def local(alm, legendre, order_ids, cycle_number, src_band, src_block, weights):
    n_band, n_ord = lax.axis_size("band"), lax.axis_size("ord")
    parts, orders, _ = alm.shape
    fields = parts // 2
    cycles = legendre.shape[0]
    cycles_here = cycle_number.shape[0]
    blocks, blk, _ = weights.shape
    npix_here = blocks * blk // cycles_here
    message = (fields * cycles + META, 2 * orders)
    cols = npix_here // blk
    q_len = min(Q_LEN, npix_here)
    vmem = pl.BlockSpec(memory_space=pltpu.VMEM)
    hbm = pl.BlockSpec(memory_space=pltpu.HBM)

    def far(*arrays):
        return [pltpu.with_memory_space_constraint(v, pltpu.HBM) for v in arrays]

    part = pl.pallas_call(
        analysis,
        name="analysis",
        out_shape=pltpu.VMEM(message, jnp.float32),
        in_specs=[hbm] * 4,
        out_specs=vmem,
        scratch_shapes=[
            pltpu.VMEM(legendre.shape, legendre.dtype),
            pltpu.VMEM(alm.shape, alm.dtype),
            pltpu.SMEM(cycle_number.shape, jnp.int32),
            pltpu.VMEM((1, orders), jnp.int32),
            pltpu.SemaphoreType.DMA((2 * (orders // GROUP) + 2,)),
        ],
        compiler_params=pltpu.CompilerParams(vmem_limit_bytes=16 << 20),
        cost_estimate=pl.CostEstimate(flops=2 << 30, bytes_accessed=6 << 20, transcendentals=0),
    )(*far(cycle_number, order_ids[None], legendre, alm))
    own, places, weights = pl.pallas_call(
        functools.partial(fetch, cycles_here, fields * cycles, cols),
        name="fetch",
        out_shape=(
            pltpu.VMEM(part.shape, part.dtype),
            pltpu.VMEM((1, blocks), jnp.int32),
            pltpu.VMEM(weights.shape, weights.dtype),
        ),
        in_specs=[vmem, vmem, vmem, hbm],
        out_specs=(vmem, vmem, vmem),
        scratch_shapes=[pltpu.VMEM(weights.shape, weights.dtype), pltpu.SemaphoreType.DMA((CHUNKS,))],
        compiler_params=pltpu.CompilerParams(vmem_limit_bytes=16 << 20),
        cost_estimate=pl.CostEstimate(flops=1 << 30, bytes_accessed=6 << 20, transcendentals=0),
    )(part, src_band.T, src_block[None], *far(weights))
    if n_band <= 8:
        total = sum(crossed(part, "band", n_band), own)
    else:
        total = lax.psum(own, "band")

    def swap(x, k):
        return lax.ppermute(x, "ord", [(i, i ^ k) for i in range(n_ord)])

    half = n_ord // 2
    here = [total] + [swap(total, k) for k in range(1, half)]
    there = swap(total, half)
    rest = [swap(there, k) for k in range(1, half)]
    synth = dict(
        out_shape=pltpu.VMEM((npix_here // q_len * fields * cycles, q_len), jnp.float32),
        out_specs=vmem,
        compiler_params=pltpu.CompilerParams(vmem_limit_bytes=16 << 20),
        cost_estimate=pl.CostEstimate(flops=1 << 30, bytes_accessed=1 << 20, transcendentals=0),
    )
    sums = pl.pallas_call(
        functools.partial(near, n_ord, fields, npix_here), name="near", in_specs=[vmem] * half, **synth
    )(*here)
    sums = pl.pallas_call(
        functools.partial(next_near, n_ord, fields, npix_here), name="next_near", in_specs=[vmem] * 2, **synth
    )(there, sums)
    pixels = (fields, cycles_here, npix_here)
    return pl.pallas_call(
        functools.partial(lens, n_ord, cycles_here, fields),
        name="lens",
        out_shape=(jax.ShapeDtypeStruct(pixels, jnp.bfloat16), jax.ShapeDtypeStruct(pixels, jnp.float32)),
        in_specs=[vmem] * (half + 2),
        out_specs=(hbm, hbm),
        scratch_shapes=[
            pltpu.VMEM((cols * fields * cycles, blk), jnp.float32),
            pltpu.VMEM((2 * cols, 16, blk), jnp.float32),
            pltpu.VMEM(pixels, jnp.bfloat16),
            pltpu.VMEM(pixels, jnp.float32),
            pltpu.SMEM((1, blocks), jnp.int32),
            pltpu.SemaphoreType.DMA((CHUNKS + 2,)),
        ],
        compiler_params=pltpu.CompilerParams(vmem_limit_bytes=32 << 20),
    )(places, *rest, sums, weights)


def solution(mesh):
    placed = (
        P("sim", "ord", "band"),
        P(None, "ord", "band"),
        P("ord"),
        P("band"),
        P(("sim", "band", "ord"), None),
        P(("sim", "band", "ord")),
        P(("sim", "band", "ord"), None, None),
    )
    return jax.shard_map(
        local,
        mesh=mesh,
        in_specs=placed,
        out_specs=(P("sim", "band", "ord"), P("sim", "band", "ord")),
        check_vma=False,
    )
```

```python
import functools

import jax
import jax.numpy as jnp
from jax import lax
from jax.experimental import pallas as pl
from jax.experimental.pallas import tpu as pltpu
from jax.sharding import PartitionSpec as P


LANES = 128
GROUP = 16
Q_LEN = 512
CHUNKS = 4
UNROLL = 32
META = 8
NT = (((1,), (1,)), ((), ()))
SINE = (6.2831851600887045, -41.34165503125142, 81.60100406374923, -76.54978209038376, 39.53670461908883)


def sin_turns(v):
    z = v * v
    total = SINE[-1]
    for term in SINE[-2::-1]:
        total = total * z + term
    return total * v


def wrap(u):
    return u - jnp.round(u)


def cos_turns(u):
    return sin_turns(0.25 - jnp.abs(u))


def split(x):
    high = x.astype(jnp.bfloat16)
    return high, (x - high.astype(jnp.float32)).astype(jnp.bfloat16)


def analysis(cycle_hbm, orders_hbm, legendre_hbm, alm_hbm, out_ref, legendre, alm, cycle_ref, orders_ref, sems):
    cycles, orders, _ = legendre.shape
    parts = alm.shape[0]
    half = parts // 2
    groups = orders // GROUP
    copies = []
    for g in range(groups):
        rows = pl.ds(g * GROUP, GROUP)
        copies.append(
            (
                pltpu.make_async_copy(alm_hbm.at[:, rows], alm.at[:, rows], sems.at[2 * g]),
                pltpu.make_async_copy(legendre_hbm.at[:, rows], legendre.at[:, rows], sems.at[2 * g + 1]),
            )
        )
    small = (
        pltpu.make_async_copy(cycle_hbm, cycle_ref, sems.at[2 * groups]),
        pltpu.make_async_copy(orders_hbm, orders_ref, sems.at[2 * groups + 1]),
    )
    for pair in copies[:1] + [small] + copies[1:]:
        for copy in pair:
            copy.start()

    for copy in small:
        copy.wait()
    band = lax.axis_index("band")
    cycles_here = cycle_ref.shape[0]
    lane = lax.broadcasted_iota(jnp.int32, (1, LANES), 1)
    parity = jnp.zeros((1, LANES), jnp.float32)
    for i in range(cycles_here):
        odd = (cycle_ref[i] & 1).astype(jnp.float32)
        parity = jnp.where(lane == band * cycles_here + i, odd, parity)
    ids = orders_ref[...].astype(jnp.float32) * jnp.where(band == 0, 1.0, 0.0)
    base = half * cycles
    out_ref[base : base + 1, :] = jnp.concatenate([ids, ids], axis=1)
    out_ref[base + 1 : base + 2, :] = parity
    out_ref[base + 2 :, :] = jnp.zeros((META - 2, LANES), jnp.float32)

    width = parts * GROUP
    share = cycles // 2
    rows_of = lax.broadcasted_iota(jnp.int32, (share * GROUP, width), 0) % GROUP
    lane_of = lax.broadcasted_iota(jnp.int32, (share * GROUP, width), 1) % GROUP
    same = rows_of == lane_of
    sums = []
    for g in range(groups):
        for copy in copies[g]:
            copy.wait()
        rows = slice(g * GROUP, (g + 1) * GROUP)
        right = alm[:, rows, :].reshape(width, -1)
        both = []
        for h in range(2):
            left = legendre[h * share : (h + 1) * share, rows, :].reshape(share * GROUP, -1)
            full = lax.dot_general(left, right, NT, preferred_element_type=jnp.float32)
            full = jnp.where(same, full, 0.0)
            both.append(jnp.sum(full.reshape(share, GROUP, width), axis=1))
        sums.append(jnp.concatenate(both, axis=0))
    for f in range(half):
        pieces = [sums[g][:, c * GROUP : (c + 1) * GROUP] for c in (f, f + half) for g in range(groups)]
        out_ref[f * cycles : (f + 1) * cycles, :] = jnp.concatenate(pieces, axis=1)


def fetch(cycles_here, rows_col, cols, part_ref, src_band_ref, src_block_ref, weights_hbm, part_out, places_ref, weights_ref, stage, sems):
    count = weights_ref.shape[0] // CHUNKS
    copies = [
        pltpu.make_async_copy(
            weights_hbm.at[pl.ds(i * count, count)], stage.at[pl.ds(i * count, count)], sems.at[i]
        )
        for i in range(CHUNKS)
    ]
    for copy in copies:
        copy.start()
    part_out[...] = part_ref[...]
    block = src_block_ref[...]
    cycle = src_band_ref[...] * cycles_here + lax.shift_right_logical(block, cols.bit_length() - 1)
    places_ref[...] = (block & (cols - 1)) * rows_col + cycle
    for i, copy in enumerate(copies):
        copy.wait()

        @pl.loop(0, count, step=UNROLL)
        def _(k):
            for j in range(UNROLL):
                weights_ref[i * count + k + j] = stage[i * count + k + j].T


def synthesis(n_ord, fields, npix_here, arrays):
    slot = lax.axis_index("ord").astype(jnp.float32)
    base = arrays[0].shape[0] - META
    cycles = base // fields
    half = LANES // 2
    npix = npix_here * n_ord
    q_len = min(Q_LEN, npix_here)
    p_len = npix_here // q_len

    ids = [a[base : base + 1] for a in arrays]
    odd = jnp.broadcast_to(arrays[0][base + 1 : base + 2], (LANES, LANES)).T[:cycles] > 0.5

    q_iota = lax.broadcasted_iota(jnp.int32, (LANES, q_len), 1).astype(jnp.float32) * (1.0 / npix)
    shift = jnp.where(lax.broadcasted_iota(jnp.int32, (LANES, q_len), 0) < half, 0.0, 0.25)
    table = []
    for m in ids:
        column = jnp.broadcast_to(m, (LANES, LANES)).T
        column = jnp.concatenate([column] * (q_len // LANES), axis=1)
        table.append(split(cos_turns(wrap(column * q_iota - shift))))
    table_high, table_low = (jnp.concatenate(v, axis=0) for v in zip(*table))

    p_iota = lax.broadcasted_iota(jnp.int32, (p_len, LANES), 0).astype(jnp.float32) * (q_len / npix)
    low_p = lax.broadcasted_iota(jnp.int32, (p_len, LANES), 1) < half
    columns = []
    for a, m in zip(arrays, ids):
        factor = jnp.where(m == 0.0, 1.0, 2.0)
        start = wrap(m * (slot * (1.0 / n_ord)))
        even_turn = wrap(wrap(m * p_iota) + start)
        odd_turn = wrap(even_turn + wrap(m * (0.5 / npix)))
        terms = []
        for turn in (even_turn, odd_turn):
            cosine = cos_turns(turn) * factor
            sine = cos_turns(wrap(turn - 0.25)) * factor
            terms.append((jnp.where(low_p, cosine, -cosine), -sine))
        x = [a[f * cycles : (f + 1) * cycles] for f in range(fields)]
        crossed_x = [pltpu.roll(v, half, 1) for v in x]
        rows = []
        for p in range(p_len):
            straight = jnp.where(odd, terms[1][0][p : p + 1], terms[0][0][p : p + 1])
            crossed = jnp.where(odd, terms[1][1][p : p + 1], terms[0][1][p : p + 1])
            rows += [x[f] * straight + crossed_x[f] * crossed for f in range(fields)]
        columns.append(split(jnp.concatenate(rows, axis=0)))
    high, low_part = (jnp.concatenate(v, axis=1) for v in zip(*columns))
    dot = functools.partial(jnp.dot, preferred_element_type=jnp.float32)
    if len(arrays) == 1:
        both = jnp.concatenate([high, low_part], axis=1)
        return dot(both, jnp.concatenate([table_high] * 2, axis=0)) + dot(high, table_low)
    return dot(high, table_high) + (dot(low_part, table_high) + dot(high, table_low))


def near(n_ord, fields, npix_here, *refs):
    refs[-1][...] = synthesis(n_ord, fields, npix_here, [r[...] for r in refs[:-1]])


def next_near(n_ord, fields, npix_here, array_ref, before_ref, out_ref):
    out_ref[...] = before_ref[...] + synthesis(n_ord, fields, npix_here, [array_ref[...]])


def lens(n_ord, cycles_here, fields, places_vmem, *refs):
    last = n_ord // 2 - 1
    arrays = refs[:last]
    near_ref, weights, sky_hbm, lensed_hbm, sky, stage, sky_out, lensed_out, places, sems = refs[last:]
    listing = pltpu.make_async_copy(places_vmem, places, sems.at[CHUNKS + 1])
    listing.start()
    band = lax.axis_index("band")
    cycles = (arrays[0].shape[0] - META) // fields
    npix_here = sky_out.shape[2]
    cols = npix_here // LANES
    q_len = near_ref.shape[1]
    p_len = npix_here // q_len
    rows_col = fields * cycles

    pixels = near_ref[...] + synthesis(n_ord, fields, npix_here, [r[...] for r in arrays])
    pixels = pixels.astype(jnp.bfloat16).astype(jnp.float32)
    for p in range(p_len):
        for j in range(q_len // LANES):
            col = p * (q_len // LANES) + j
            sky[col * rows_col : (col + 1) * rows_col, :] = pixels[
                p * rows_col : (p + 1) * rows_col, j * LANES : (j + 1) * LANES
            ]

    first = pl.multiple_of(band * cycles_here, cycles_here)
    for col in range(cols):
        for f in range(fields):
            own = sky[pl.ds(col * rows_col + f * cycles + first, cycles_here), :]
            sky_out[f, :, col * LANES : (col + 1) * LANES] = own.astype(jnp.bfloat16)
    copies = [pltpu.make_async_copy(sky_out, sky_hbm, sems.at[0])]
    copies[0].start()

    listing.wait()
    stage[...] = jnp.zeros_like(stage)
    for col in range(cols):
        for c in range(cycles_here):
            source = sky[pl.ds(places[0, c * cols + col], fields, stride=cycles), :]
            stage[2 * col + c % 2, pl.ds(c, fields, stride=cycles_here), :] = source

    rows = stage.shape[1]
    cycle_of = lax.broadcasted_iota(jnp.int32, (rows, LANES), 0) % cycles_here
    chunk = cols // CHUNKS
    for col in range(cols):
        left = jnp.concatenate([stage[2 * col], stage[2 * col + 1]], axis=1).astype(jnp.bfloat16)
        right = jnp.concatenate(
            [
                jnp.concatenate([weights[c * cols + col] for c in range(n, cycles_here, 2)], axis=1)
                for n in range(2)
            ],
            axis=0,
        )
        full = jnp.dot(left, right, preferred_element_type=jnp.float32)
        out = full[:, 0:LANES]
        for n in range(1, cycles_here // 2):
            out = jnp.where(cycle_of // 2 == n, full[:, n * LANES : (n + 1) * LANES], out)
        for f in range(fields):
            lensed_out[f, :, col * LANES : (col + 1) * LANES] = out[f * cycles_here : (f + 1) * cycles_here]
        if (col + 1) % chunk == 0:
            lanes = pl.ds((col + 1 - chunk) * LANES, chunk * LANES)
            copies.append(
                pltpu.make_async_copy(
                    lensed_out.at[:, :, lanes], lensed_hbm.at[:, :, lanes], sems.at[(col + 1) // chunk]
                )
            )
            copies[-1].start()
    for copy in copies:
        copy.wait()


def shifted(x, axis, n):
    out = []
    for k in range(1, n):
        out.append(lax.ppermute(x, axis, [(i, (i + k) % n) for i in range(n)]))
    return out


def local(alm, legendre, order_ids, cycle_number, src_band, src_block, weights):
    n_band, n_ord = lax.axis_size("band"), lax.axis_size("ord")
    parts, orders, _ = alm.shape
    fields = parts // 2
    cycles = legendre.shape[0]
    cycles_here = cycle_number.shape[0]
    blocks, blk, _ = weights.shape
    npix_here = blocks * blk // cycles_here
    message = (fields * cycles + META, 2 * orders)
    cols = npix_here // blk
    q_len = min(Q_LEN, npix_here)
    vmem = pl.BlockSpec(memory_space=pltpu.VMEM)
    hbm = pl.BlockSpec(memory_space=pltpu.HBM)

    def far(*arrays):
        return [pltpu.with_memory_space_constraint(v, pltpu.HBM) for v in arrays]

    part = pl.pallas_call(
        analysis,
        name="analysis",
        out_shape=pltpu.VMEM(message, jnp.float32),
        in_specs=[hbm] * 4,
        out_specs=vmem,
        scratch_shapes=[
            pltpu.VMEM(legendre.shape, legendre.dtype),
            pltpu.VMEM(alm.shape, alm.dtype),
            pltpu.SMEM(cycle_number.shape, jnp.int32),
            pltpu.VMEM((1, orders), jnp.int32),
            pltpu.SemaphoreType.DMA((2 * (orders // GROUP) + 2,)),
        ],
        compiler_params=pltpu.CompilerParams(vmem_limit_bytes=16 << 20),
        cost_estimate=pl.CostEstimate(flops=2 << 30, bytes_accessed=6 << 20, transcendentals=0),
    )(*far(cycle_number, order_ids[None], legendre, alm))
    own, places, weights = pl.pallas_call(
        functools.partial(fetch, cycles_here, fields * cycles, cols),
        name="fetch",
        out_shape=(
            pltpu.VMEM(part.shape, part.dtype),
            pltpu.VMEM((1, blocks), jnp.int32),
            pltpu.VMEM(weights.shape, weights.dtype),
        ),
        in_specs=[vmem, vmem, vmem, hbm],
        out_specs=(vmem, vmem, vmem),
        scratch_shapes=[pltpu.VMEM(weights.shape, weights.dtype), pltpu.SemaphoreType.DMA((CHUNKS,))],
        compiler_params=pltpu.CompilerParams(vmem_limit_bytes=16 << 20),
        cost_estimate=pl.CostEstimate(flops=1 << 30, bytes_accessed=6 << 20, transcendentals=0),
    )(part, src_band.T, src_block[None], *far(weights))
    if n_band <= 8:
        total = sum(shifted(part, "band", n_band), own)
    else:
        total = lax.psum(own, "band")

    def swap(x, k):
        return lax.ppermute(x, "ord", [(i, i ^ k) for i in range(n_ord)])

    half = n_ord // 2
    here = [total] + [swap(total, k) for k in range(1, half)]
    there = swap(total, half)
    rest = [swap(there, k) for k in range(1, half)]
    synth = dict(
        out_shape=pltpu.VMEM((npix_here // q_len * fields * cycles, q_len), jnp.float32),
        out_specs=vmem,
        compiler_params=pltpu.CompilerParams(vmem_limit_bytes=16 << 20),
        cost_estimate=pl.CostEstimate(flops=1 << 30, bytes_accessed=1 << 20, transcendentals=0),
    )
    sums = pl.pallas_call(
        functools.partial(near, n_ord, fields, npix_here), name="near", in_specs=[vmem] * half, **synth
    )(*here)
    sums = pl.pallas_call(
        functools.partial(next_near, n_ord, fields, npix_here), name="next_near", in_specs=[vmem] * 2, **synth
    )(there, sums)
    pixels = (fields, cycles_here, npix_here)
    return pl.pallas_call(
        functools.partial(lens, n_ord, cycles_here, fields),
        name="lens",
        out_shape=(jax.ShapeDtypeStruct(pixels, jnp.bfloat16), jax.ShapeDtypeStruct(pixels, jnp.float32)),
        in_specs=[vmem] * (half + 2),
        out_specs=(hbm, hbm),
        scratch_shapes=[
            pltpu.VMEM((cols * fields * cycles, blk), jnp.float32),
            pltpu.VMEM((2 * cols, 16, blk), jnp.float32),
            pltpu.VMEM(pixels, jnp.bfloat16),
            pltpu.VMEM(pixels, jnp.float32),
            pltpu.SMEM((1, blocks), jnp.int32),
            pltpu.SemaphoreType.DMA((CHUNKS + 2,)),
        ],
        compiler_params=pltpu.CompilerParams(vmem_limit_bytes=32 << 20),
    )(places, *rest, sums, weights)


def solution(mesh):
    placed = (
        P("sim", "ord", "band"),
        P(None, "ord", "band"),
        P("ord"),
        P("band"),
        P(("sim", "band", "ord"), None),
        P(("sim", "band", "ord")),
        P(("sim", "band", "ord"), None, None),
    )
    return jax.shard_map(
        local,
        mesh=mesh,
        in_specs=placed,
        out_specs=(P("sim", "band", "ord"), P("sim", "band", "ord")),
        check_vma=False,
    )
```

```python
import functools

import jax
import jax.numpy as jnp
from jax import lax
from jax.experimental import pallas as pl
from jax.experimental.pallas import tpu as pltpu
from jax.sharding import PartitionSpec as P


LANES = 128
GROUP = 16
Q_LEN = 512
CHUNKS = 4
UNROLL = 32
META = 8
NT = (((1,), (1,)), ((), ()))
SINE = (6.2831851600887045, -41.34165503125142, 81.60100406374923, -76.54978209038376, 39.53670461908883)


def sin_turns(v):
    z = v * v
    total = SINE[-1]
    for term in SINE[-2::-1]:
        total = total * z + term
    return total * v


def wrap(u):
    return u - jnp.round(u)


def cos_turns(u):
    return sin_turns(0.25 - jnp.abs(u))


def split(x):
    high = x.astype(jnp.bfloat16)
    return high, (x - high.astype(jnp.float32)).astype(jnp.bfloat16)


def analysis(cycle_hbm, orders_hbm, legendre_hbm, alm_hbm, out_ref, legendre, alm, cycle_ref, orders_ref, sems):
    cycles, orders, _ = legendre.shape
    parts = alm.shape[0]
    half = parts // 2
    groups = orders // GROUP
    copies = []
    for g in range(groups):
        rows = pl.ds(g * GROUP, GROUP)
        copies.append(
            (
                pltpu.make_async_copy(alm_hbm.at[:, rows], alm.at[:, rows], sems.at[2 * g]),
                pltpu.make_async_copy(legendre_hbm.at[:, rows], legendre.at[:, rows], sems.at[2 * g + 1]),
            )
        )
    small = (
        pltpu.make_async_copy(cycle_hbm, cycle_ref, sems.at[2 * groups]),
        pltpu.make_async_copy(orders_hbm, orders_ref, sems.at[2 * groups + 1]),
    )
    for pair in copies[:1] + [small] + copies[1:]:
        for copy in pair:
            copy.start()

    for copy in small:
        copy.wait()
    band = lax.axis_index("band")
    cycles_here = cycle_ref.shape[0]
    lane = lax.broadcasted_iota(jnp.int32, (1, LANES), 1)
    parity = jnp.zeros((1, LANES), jnp.float32)
    for i in range(cycles_here):
        odd = (cycle_ref[i] & 1).astype(jnp.float32)
        parity = jnp.where(lane == band * cycles_here + i, odd, parity)
    ids = orders_ref[...].astype(jnp.float32) * jnp.where(band == 0, 1.0, 0.0)
    base = half * cycles
    out_ref[base : base + 1, :] = jnp.concatenate([ids, ids], axis=1)
    out_ref[base + 1 : base + 2, :] = parity
    out_ref[base + 2 :, :] = jnp.zeros((META - 2, LANES), jnp.float32)

    width = parts * GROUP
    share = cycles // 2
    rows_of = lax.broadcasted_iota(jnp.int32, (share * GROUP, width), 0) % GROUP
    lane_of = lax.broadcasted_iota(jnp.int32, (share * GROUP, width), 1) % GROUP
    same = rows_of == lane_of
    sums = []
    for g in range(groups):
        for copy in copies[g]:
            copy.wait()
        rows = slice(g * GROUP, (g + 1) * GROUP)
        right = alm[:, rows, :].reshape(width, -1)
        both = []
        for h in range(2):
            left = legendre[h * share : (h + 1) * share, rows, :].reshape(share * GROUP, -1)
            full = lax.dot_general(left, right, NT, preferred_element_type=jnp.float32)
            full = jnp.where(same, full, 0.0)
            both.append(jnp.sum(full.reshape(share, GROUP, width), axis=1))
        sums.append(jnp.concatenate(both, axis=0))
    for f in range(half):
        pieces = [sums[g][:, c * GROUP : (c + 1) * GROUP] for c in (f, f + half) for g in range(groups)]
        out_ref[f * cycles : (f + 1) * cycles, :] = jnp.concatenate(pieces, axis=1)


def fetch(cycles_here, rows_col, cols, part_ref, src_band_ref, src_block_ref, weights_hbm, part_out, places_ref, weights_ref, rest_ref, stage, sems):
    count = rest_ref.shape[0]
    copies = [
        pltpu.make_async_copy(
            weights_hbm.at[pl.ds(i * count, count)],
            stage.at[pl.ds(i * count, count)] if i < CHUNKS - 1 else rest_ref,
            sems.at[i],
        )
        for i in range(CHUNKS)
    ]
    for copy in copies:
        copy.start()
    part_out[...] = part_ref[...]
    block = src_block_ref[...]
    cycle = src_band_ref[...] * cycles_here + lax.shift_right_logical(block, cols.bit_length() - 1)
    places_ref[...] = (block & (cols - 1)) * rows_col + cycle
    for i, copy in enumerate(copies[:-1]):
        copy.wait()

        @pl.loop(0, count, step=UNROLL)
        def _(k):
            for j in range(UNROLL):
                weights_ref[i * count + k + j] = stage[i * count + k + j].T

    copies[-1].wait()


def synthesis(n_ord, fields, npix_here, arrays):
    slot = lax.axis_index("ord").astype(jnp.float32)
    base = arrays[0].shape[0] - META
    cycles = base // fields
    half = LANES // 2
    npix = npix_here * n_ord
    q_len = min(Q_LEN, npix_here)
    p_len = npix_here // q_len

    ids = [a[base : base + 1] for a in arrays]
    odd = jnp.broadcast_to(arrays[0][base + 1 : base + 2], (LANES, LANES)).T[:cycles] > 0.5

    q_iota = lax.broadcasted_iota(jnp.int32, (LANES, q_len), 1).astype(jnp.float32) * (1.0 / npix)
    shift = jnp.where(lax.broadcasted_iota(jnp.int32, (LANES, q_len), 0) < half, 0.0, 0.25)
    table = []
    for m in ids:
        column = jnp.broadcast_to(m, (LANES, LANES)).T
        column = jnp.concatenate([column] * (q_len // LANES), axis=1)
        table.append(split(cos_turns(wrap(column * q_iota - shift))))
    table_high, table_low = (jnp.concatenate(v, axis=0) for v in zip(*table))

    p_iota = lax.broadcasted_iota(jnp.int32, (p_len, LANES), 0).astype(jnp.float32) * (q_len / npix)
    low_p = lax.broadcasted_iota(jnp.int32, (p_len, LANES), 1) < half
    columns = []
    for a, m in zip(arrays, ids):
        factor = jnp.where(m == 0.0, 1.0, 2.0)
        start = wrap(m * (slot * (1.0 / n_ord)))
        even_turn = wrap(wrap(m * p_iota) + start)
        odd_turn = wrap(even_turn + wrap(m * (0.5 / npix)))
        terms = []
        for turn in (even_turn, odd_turn):
            cosine = cos_turns(turn) * factor
            sine = cos_turns(wrap(turn - 0.25)) * factor
            terms.append((jnp.where(low_p, cosine, -cosine), -sine))
        x = [a[f * cycles : (f + 1) * cycles] for f in range(fields)]
        crossed_x = [pltpu.roll(v, half, 1) for v in x]
        rows = []
        for p in range(p_len):
            straight = jnp.where(odd, terms[1][0][p : p + 1], terms[0][0][p : p + 1])
            crossed = jnp.where(odd, terms[1][1][p : p + 1], terms[0][1][p : p + 1])
            rows += [x[f] * straight + crossed_x[f] * crossed for f in range(fields)]
        columns.append(split(jnp.concatenate(rows, axis=0)))
    high, low_part = (jnp.concatenate(v, axis=1) for v in zip(*columns))
    dot = functools.partial(jnp.dot, preferred_element_type=jnp.float32)
    if len(arrays) == 1:
        both = jnp.concatenate([high, low_part], axis=1)
        return dot(both, jnp.concatenate([table_high] * 2, axis=0)) + dot(high, table_low)
    return dot(high, table_high) + (dot(low_part, table_high) + dot(high, table_low))


def near(n_ord, fields, npix_here, *refs):
    rest, out, turned = refs[-3:]
    out[...] = synthesis(n_ord, fields, npix_here, [r[...] for r in refs[:-3]])

    @pl.loop(0, rest.shape[0], step=UNROLL)
    def _(k):
        for j in range(UNROLL):
            turned[k + j] = rest[k + j].T


def next_near(n_ord, fields, npix_here, array_ref, before_ref, out_ref):
    out_ref[...] = before_ref[...] + synthesis(n_ord, fields, npix_here, [array_ref[...]])


def lens(n_ord, cycles_here, fields, places_vmem, *refs):
    last = n_ord // 2 - 1
    arrays = refs[:last]
    near_ref, weights_a, weights_b, sky_hbm, lensed_hbm, sky, stage, sky_out, lensed_out, places, sems = refs[last:]
    listing = pltpu.make_async_copy(places_vmem, places, sems.at[CHUNKS + 1])
    listing.start()
    stage[...] = jnp.zeros_like(stage)
    weights = [w.at[i] for w in (weights_a, weights_b) for i in range(w.shape[0])]
    band = lax.axis_index("band")
    cycles = (arrays[0].shape[0] - META) // fields
    npix_here = sky_out.shape[2]
    cols = npix_here // LANES
    q_len = near_ref.shape[1]
    p_len = npix_here // q_len
    rows_col = fields * cycles

    pixels = near_ref[...] + synthesis(n_ord, fields, npix_here, [r[...] for r in arrays])
    pixels = pixels.astype(jnp.bfloat16).astype(jnp.float32)
    for p in range(p_len):
        for j in range(q_len // LANES):
            col = p * (q_len // LANES) + j
            sky[col * rows_col : (col + 1) * rows_col, :] = pixels[
                p * rows_col : (p + 1) * rows_col, j * LANES : (j + 1) * LANES
            ]

    first = pl.multiple_of(band * cycles_here, cycles_here)
    for col in range(cols):
        for f in range(fields):
            own = sky[pl.ds(col * rows_col + f * cycles + first, cycles_here), :]
            sky_out[f, :, col * LANES : (col + 1) * LANES] = own.astype(jnp.bfloat16)
    copies = [pltpu.make_async_copy(sky_out, sky_hbm, sems.at[0])]
    copies[0].start()

    listing.wait()
    for col in range(cols):
        for c in range(cycles_here):
            source = sky[pl.ds(places[0, c * cols + col], fields, stride=cycles), :]
            stage[2 * col + c % 2, pl.ds(c, fields, stride=cycles_here), :] = source

    rows = stage.shape[1]
    cycle_of = lax.broadcasted_iota(jnp.int32, (rows, LANES), 0) % cycles_here
    chunk = cols // CHUNKS
    for col in range(cols):
        left = jnp.concatenate([stage[2 * col], stage[2 * col + 1]], axis=1).astype(jnp.bfloat16)
        right = jnp.concatenate(
            [
                jnp.concatenate([weights[c * cols + col][...] for c in range(n, cycles_here, 2)], axis=1)
                for n in range(2)
            ],
            axis=0,
        )
        full = jnp.dot(left, right, preferred_element_type=jnp.float32)
        out = full[:, 0:LANES]
        for n in range(1, cycles_here // 2):
            out = jnp.where(cycle_of // 2 == n, full[:, n * LANES : (n + 1) * LANES], out)
        for f in range(fields):
            lensed_out[f, :, col * LANES : (col + 1) * LANES] = out[f * cycles_here : (f + 1) * cycles_here]
        if (col + 1) % chunk == 0:
            lanes = pl.ds((col + 1 - chunk) * LANES, chunk * LANES)
            copies.append(
                pltpu.make_async_copy(
                    lensed_out.at[:, :, lanes], lensed_hbm.at[:, :, lanes], sems.at[(col + 1) // chunk]
                )
            )
            copies[-1].start()
    for copy in copies:
        copy.wait()


def shifted(x, axis, n):
    out = []
    for k in range(1, n):
        out.append(lax.ppermute(x, axis, [(i, (i + k) % n) for i in range(n)]))
    return out


def local(alm, legendre, order_ids, cycle_number, src_band, src_block, weights):
    n_band, n_ord = lax.axis_size("band"), lax.axis_size("ord")
    parts, orders, _ = alm.shape
    fields = parts // 2
    cycles = legendre.shape[0]
    cycles_here = cycle_number.shape[0]
    blocks, blk, _ = weights.shape
    npix_here = blocks * blk // cycles_here
    message = (fields * cycles + META, 2 * orders)
    cols = npix_here // blk
    q_len = min(Q_LEN, npix_here)
    vmem = pl.BlockSpec(memory_space=pltpu.VMEM)
    hbm = pl.BlockSpec(memory_space=pltpu.HBM)

    def far(*arrays):
        return [pltpu.with_memory_space_constraint(v, pltpu.HBM) for v in arrays]

    part = pl.pallas_call(
        analysis,
        name="analysis",
        out_shape=pltpu.VMEM(message, jnp.float32),
        in_specs=[hbm] * 4,
        out_specs=vmem,
        scratch_shapes=[
            pltpu.VMEM(legendre.shape, legendre.dtype),
            pltpu.VMEM(alm.shape, alm.dtype),
            pltpu.SMEM(cycle_number.shape, jnp.int32),
            pltpu.VMEM((1, orders), jnp.int32),
            pltpu.SemaphoreType.DMA((2 * (orders // GROUP) + 2,)),
        ],
        compiler_params=pltpu.CompilerParams(vmem_limit_bytes=16 << 20),
        cost_estimate=pl.CostEstimate(flops=2 << 30, bytes_accessed=6 << 20, transcendentals=0),
    )(*far(cycle_number, order_ids[None], legendre, alm))
    few = (blocks // CHUNKS, blk, blk)
    most = (blocks - few[0], blk, blk)
    own, places, weights_a, weights_b = pl.pallas_call(
        functools.partial(fetch, cycles_here, fields * cycles, cols),
        name="fetch",
        out_shape=(
            pltpu.VMEM(part.shape, part.dtype),
            pltpu.VMEM((1, blocks), jnp.int32),
            pltpu.VMEM(most, weights.dtype),
            pltpu.VMEM(few, weights.dtype),
        ),
        in_specs=[vmem, vmem, vmem, hbm],
        out_specs=(vmem,) * 4,
        scratch_shapes=[pltpu.VMEM(most, weights.dtype), pltpu.SemaphoreType.DMA((CHUNKS,))],
        compiler_params=pltpu.CompilerParams(vmem_limit_bytes=16 << 20),
        cost_estimate=pl.CostEstimate(flops=1 << 30, bytes_accessed=6 << 20, transcendentals=0),
    )(part, src_band.T, src_block[None], *far(weights))
    if n_band <= 8:
        total = sum(shifted(part, "band", n_band), own)
    else:
        total = lax.psum(own, "band")

    def swap(x, k):
        return lax.ppermute(x, "ord", [(i, i ^ k) for i in range(n_ord)])

    half = n_ord // 2
    here = [total] + [swap(total, k) for k in range(1, half)]
    there = swap(total, half)
    rest = [swap(there, k) for k in range(1, half)]
    synth = dict(
        compiler_params=pltpu.CompilerParams(vmem_limit_bytes=16 << 20),
        cost_estimate=pl.CostEstimate(flops=1 << 30, bytes_accessed=1 << 20, transcendentals=0),
    )
    partial_sky = pltpu.VMEM((npix_here // q_len * fields * cycles, q_len), jnp.float32)
    sums, weights_b = pl.pallas_call(
        functools.partial(near, n_ord, fields, npix_here),
        name="near",
        in_specs=[vmem] * (half + 1),
        out_shape=(partial_sky, pltpu.VMEM(few, weights.dtype)),
        out_specs=(vmem, vmem),
        **synth,
    )(*here, weights_b)
    sums = pl.pallas_call(
        functools.partial(next_near, n_ord, fields, npix_here),
        name="next_near",
        in_specs=[vmem] * 2,
        out_shape=partial_sky,
        out_specs=vmem,
        **synth,
    )(there, sums)
    pixels = (fields, cycles_here, npix_here)
    return pl.pallas_call(
        functools.partial(lens, n_ord, cycles_here, fields),
        name="lens",
        out_shape=(jax.ShapeDtypeStruct(pixels, jnp.bfloat16), jax.ShapeDtypeStruct(pixels, jnp.float32)),
        in_specs=[vmem] * (half + 3),
        out_specs=(hbm, hbm),
        scratch_shapes=[
            pltpu.VMEM((cols * fields * cycles, blk), jnp.float32),
            pltpu.VMEM((2 * cols, 16, blk), jnp.float32),
            pltpu.VMEM(pixels, jnp.bfloat16),
            pltpu.VMEM(pixels, jnp.float32),
            pltpu.SMEM((1, blocks), jnp.int32),
            pltpu.SemaphoreType.DMA((CHUNKS + 2,)),
        ],
        compiler_params=pltpu.CompilerParams(vmem_limit_bytes=32 << 20),
    )(places, *rest, sums, weights_a, weights_b)


def solution(mesh):
    placed = (
        P("sim", "ord", "band"),
        P(None, "ord", "band"),
        P("ord"),
        P("band"),
        P(("sim", "band", "ord"), None),
        P(("sim", "band", "ord")),
        P(("sim", "band", "ord"), None, None),
    )
    return jax.shard_map(
        local,
        mesh=mesh,
        in_specs=placed,
        out_specs=(P("sim", "band", "ord"), P("sim", "band", "ord")),
        check_vma=False,
    )
```
